512 devices in a mesh: leaf: 128 (over z, y, core), sub: 4 (over x).
Axes of the slice: x: 4, y: 8, z: 8, core: 2. Of those that a mesh axis runs over, the one named last changes fastest.
Arguments:
- signal: bfloat16 [32, 1048576], P(None, ('leaf', 'sub')), may hold values from -6 to 6
- row_basis: bfloat16 [64, 1048576], P(None, ('leaf', 'sub')), may hold values from -0.375 to 0.375
- transfer: bfloat16 [8192, 13, 32, 128], P(('leaf', 'sub')), may hold values from -0.5 to 0.5
- column_basis: bfloat16 [64, 1048576], P(None, ('leaf', 'sub')), may hold values from -0.75 to 0.75
- near_blocks: bfloat16 [12288, 128, 256], P(('leaf', 'sub')), may hold values from -0.375 to 0.375
- near_list: int32 [12288, 2], P(('leaf', 'sub')), may hold values from -1 to 31, as said below
Outputs:
- result: float32 [32, 1048576], P(None, ('leaf', 'sub'))
The draws below stay inside these ranges and needn't reach their ends.
Inputs may be any that keep to these rules, and one draw needn't show every extreme that they name: `near_list`: on each device the live entries (column >= 0) fill a leading run of its 24 slots, 2 or more of them, and empty slots hold -1 in both places; a live entry has 0 <= column < 24 and column <= row <= column + 8. Devices 2m and 2m + 1 hold at most 24 live entries together, and some such pair holds 24.
All inputs are finite; a program needn't handle non-finite values.
Results may differ from the reference program's by a relative error of at most 0.0003.
Values may be sent and summed in bfloat16 or wider, within the bound.
A program may use at most 128 MiB of HBM per device.

```python
import jax
import jax.numpy as jnp
from jax import lax

BLOCK_RANK = 32
RHS = 16
LEAF = 128
BOX_DEV = 16
REACH = 4
CAP = 24
BUTTERFLY_DEPTH = 13
TOTAL_LEAF_BOXES = 8192
NPTS = 1048576
NEAR_SLOTS = 12288
DEVICES = 512


def draw_near_list(key, part):
    pair_count = DEVICES // 2
    subkeys = jax.random.split(key, 6)
    heavy_count = jax.random.randint(subkeys[0], (pair_count,), CAP // 2, CAP - 1)
    full_pair = jax.random.randint(subkeys[1], (), 0, pair_count)
    heavy_count = jnp.where(jnp.arange(pair_count) == full_pair, CAP - 2, heavy_count)
    spare_room = CAP - heavy_count
    light_count = jax.random.randint(subkeys[2], (pair_count,), 2, spare_room + 1)
    heavy_first = jax.random.randint(subkeys[3], (pair_count,), 0, 2)
    first_count = jnp.where(heavy_first == 0, heavy_count, light_count)
    second_count = jnp.where(heavy_first == 0, light_count, heavy_count)
    counts = jnp.stack([first_count, second_count], axis=1).reshape(DEVICES)
    col_index = jax.random.randint(subkeys[4], (DEVICES, CAP), 0, BOX_DEV + 2 * REACH)
    offsets = jax.random.randint(subkeys[5], (DEVICES, CAP), 0, 2 * REACH + 1)
    slot_ids = jnp.arange(CAP)[None, :]
    col_index = jnp.where(slot_ids == 0, 0, col_index)
    offsets = jnp.where(slot_ids == 0, offsets % (2 * REACH), offsets)
    col_index = jnp.where(slot_ids == 1, BOX_DEV + 2 * REACH - 1, col_index)
    offsets = jnp.where(slot_ids == 1, 2 * REACH, offsets)
    row_index = col_index + offsets
    live_slot = slot_ids < counts[:, None]
    col_index = jnp.where(live_slot, col_index, -1)
    row_index = jnp.where(live_slot, row_index, -1)
    return jnp.stack([row_index, col_index], axis=-1).reshape(DEVICES * CAP, 2).astype(jnp.int32)


def shard_levels(own_key, extent, shards, smallest, high):
    def one(axis_at, parts):
        draws = jax.random.uniform(jax.random.fold_in(jax.random.fold_in(own_key, 6), axis_at), (parts,), jnp.float32, smallest / len(shards), high / len(shards))
        return jnp.repeat(jnp.exp(draws), extent[axis_at] // parts).reshape((-1,) + (1,) * (len(extent) - axis_at - 1))

    loudness = one(*shards[0])
    for cut in shards[1:]:
        loudness = loudness * one(*cut)
    return loudness


def gaussian(own_key, extent, deviation, reach, cuts=(), kind=jnp.bfloat16):
    level = shard_levels(own_key, extent, cuts, -0.22, 0.18) if cuts else 1.0
    drawn = jax.random.normal(own_key, extent, jnp.float32) * deviation * level
    return jnp.minimum(jnp.maximum(drawn, -reach), reach).astype(kind)


def setup_inputs(seed: int = 0) -> dict:
    streams_of = jax.random.split(jax.random.key(seed), 7)
    return {
        "signal": gaussian(streams_of[0], (2 * RHS, NPTS), 1.0, 6.0, ((1, 512),)),
        "row_basis": gaussian(streams_of[1], (2 * BLOCK_RANK, NPTS), (2 * LEAF) ** -0.5, 0.375, ((1, 512),)),
        "transfer": gaussian(streams_of[2], (TOTAL_LEAF_BOXES, BUTTERFLY_DEPTH, BLOCK_RANK, 4 * BLOCK_RANK), (4 * BLOCK_RANK) ** -0.5, 0.5, ((0, 512),)),
        "column_basis": gaussian(streams_of[3], (2 * BLOCK_RANK, NPTS), (2 * BLOCK_RANK) ** -0.5, 0.75, ((1, 512),)),
        "near_blocks": gaussian(streams_of[4], (NEAR_SLOTS, LEAF, 2 * LEAF), (2 * LEAF) ** -0.5, 0.375, ((0, 512),)),
        "near_list": draw_near_list(jax.random.fold_in(streams_of[6], 71), 0),
    }


highest = lax.Precision.HIGHEST


def project(signal, row_basis):
    rhs_count = signal.shape[0] // 2
    rank_width = row_basis.shape[0] // 2
    leaves = signal.shape[1] // LEAF
    samples = signal.astype(jnp.float32).reshape(2, rhs_count, leaves, LEAF)
    basis_rows = row_basis.astype(jnp.float32).reshape(2, rank_width, leaves, LEAF)
    products = jnp.einsum('xrlp,yqlp->xylrq', samples, basis_rows)
    real_part = products[0, 0] + products[1, 1]
    imag_part = products[1, 0] - products[0, 1]
    return jnp.transpose(jnp.concatenate([real_part, imag_part], axis=-1), (1, 0, 2))


def block_form(weights):
    matrices = weights.astype(jnp.float32)
    rank_width = matrices.shape[1]
    pieces = []
    for offspring in range(2):
        real_part = matrices[:, :, (2 * offspring) * rank_width:(2 * offspring + 1) * rank_width]
        imag_part = matrices[:, :, (2 * offspring + 1) * rank_width:(2 * offspring + 2) * rank_width]
        upper_rows = jnp.concatenate([real_part, -imag_part], axis=2)
        lower_rows = jnp.concatenate([imag_part, real_part], axis=2)
        pieces.append(jnp.concatenate([upper_rows, lower_rows], axis=1))
    return jnp.concatenate(pieces, axis=1)


def apply_level(paired, weights):
    return jnp.einsum('rsm,smn->rsn', paired, block_form(weights), precision=highest)


def pair_local(coeffs, height):
    rhs_count, slot_count, doubled = coeffs.shape
    half_span = 2 ** (height - 1)
    grouped = coeffs.reshape(rhs_count, slot_count // (2 * half_span), 2, half_span, doubled)
    joined = jnp.concatenate([grouped[:, :, 0], grouped[:, :, 1]], axis=-1)
    twice = jnp.stack([joined, joined], axis=2)
    return twice.reshape(rhs_count, slot_count, 2 * doubled)


def evaluate(coeffs, column_basis):
    rhs_count, leaves, doubled = coeffs.shape
    rank_width = doubled // 2
    basis_rows = column_basis.astype(jnp.float32).reshape(2, rank_width, leaves, LEAF)
    real_coefficient = coeffs[:, :, :rank_width]
    imag_coef = coeffs[:, :, rank_width:]
    real_out = (jnp.einsum('rlq,qlp->rlp', real_coefficient, basis_rows[0], precision=highest)
                - jnp.einsum('rlq,qlp->rlp', imag_coef, basis_rows[1], precision=highest))
    imag_out = (jnp.einsum('rlq,qlp->rlp', imag_coef, basis_rows[0], precision=highest)
                + jnp.einsum('rlq,qlp->rlp', real_coefficient, basis_rows[1], precision=highest))
    return jnp.concatenate([real_out, imag_out], axis=0).reshape(2 * rhs_count, leaves * LEAF)


def pick_rows(window, row_index):
    channels = window.shape[0]
    leaf_tiles = window.reshape(channels, -1, LEAF)
    picked = jnp.take(leaf_tiles, jnp.maximum(row_index, 0), axis=1)
    return jnp.transpose(picked, (1, 0, 2))


def near_products(picked, blocks):
    products = jnp.einsum('scp,spj->scj', picked.astype(jnp.float32), blocks.astype(jnp.float32))
    rhs_count = picked.shape[1] // 2
    real_part = products[:, :rhs_count, :LEAF] + products[:, rhs_count:, LEAF:]
    imag_part = products[:, rhs_count:, :LEAF] - products[:, :rhs_count, LEAF:]
    return jnp.concatenate([real_part, imag_part], axis=1)


def accumulate(output_values, col_index, box_count):
    selector = (col_index[:, None] == jnp.arange(box_count, dtype=jnp.int32)[None, :]).astype(jnp.float32)
    return jnp.einsum('sw,scj->cwj', selector, output_values, precision=highest)


def near_field(signal, near_blocks, near_list):
    channels = signal.shape[0]
    window_width = (BOX_DEV + 4 * REACH) * LEAF
    edge_width = 2 * REACH * LEAF
    extended = jnp.concatenate([signal[:, -edge_width:], signal, signal[:, :edge_width]], axis=1)
    blocks = near_blocks.reshape(DEVICES, CAP, LEAF, 2 * LEAF)
    entries = near_list.reshape(DEVICES, CAP, 2)

    def one_device(item_data):
        device, dev_blocks, dev_entries = item_data
        window = lax.dynamic_slice_in_dim(extended, device * (BOX_DEV * LEAF), window_width, 1)
        picked = pick_rows(window, dev_entries[:, 0])
        return accumulate(near_products(picked, dev_blocks), dev_entries[:, 1], BOX_DEV + 2 * REACH)

    windows = lax.map(one_device, (jnp.arange(DEVICES, dtype=jnp.int32), blocks, entries))
    center = windows[:, :, REACH:REACH + BOX_DEV]
    left_rim = windows[:, :, :REACH]
    right_rim = windows[:, :, BOX_DEV + REACH:]
    center = center.at[:, :, BOX_DEV - REACH:].add(jnp.roll(left_rim, -1, axis=0))
    center = center.at[:, :, :REACH].add(jnp.roll(right_rim, 1, axis=0))
    return jnp.transpose(center, (1, 0, 2, 3)).reshape(channels, DEVICES * BOX_DEV * LEAF)


def reference(signal, row_basis, transfer, column_basis, near_blocks, near_list):
    coeffs = project(signal, row_basis)
    for height in range(1, BUTTERFLY_DEPTH + 1):
        coeffs = apply_level(pair_local(coeffs, height), transfer[:, height - 1])
    far_field = evaluate(coeffs, column_basis)
    return far_field + near_field(signal, near_blocks, near_list)
```

```python
import functools

import jax
import jax.numpy as jnp
from jax import lax
from jax.experimental import pallas as pl
from jax.experimental.pallas import tpu as pltpu
from jax.sharding import PartitionSpec as P

LEAF = 128
BOXES = 16
PAIRS = 8
RHS = 16
CAP = 24
REACH = 4
LEVELS = 13
LOCAL = 4
PHASES = (
    ("sub", (0, 1)),
    ("leaf", (0,)),
    ("leaf", (1,)),
    ("leaf", (2, 3)),
    ("leaf", (4,)),
    ("leaf", (5, 6)),
)
WIRE = "f32"

BF = jnp.bfloat16
F32 = jnp.float32
MESH = pl.DeviceIdType.MESH


def bit_of(index, bit):
    return (index // (1 << bit)) % 2


def flipped(index, bit):
    return index + (1 - 2 * bit_of(index, bit)) * (1 << bit)


def pieces(values):
    high = values.astype(BF)
    low = (values - high.astype(F32)).astype(BF)
    return jnp.concatenate([high, low], axis=0)


def folded(product):
    half = product.shape[0] // 2
    return product[:half] + product[half:]


def dot(left, right):
    return jnp.dot(left, right, preferred_element_type=F32)


def phase_plan():
    plan = []
    level = LOCAL
    slot = 0
    for axis, bits in PHASES:
        if len(bits) == 1:
            plan.append((axis, bits, level, ((bits[0],),), None))
        else:
            low, high = bits
            plan.append((axis, bits, level, ((high,), (low, high), (low,)), slot))
            slot += 1
        level += len(bits)
    return tuple(plan), slot


PLAN, MERGED = phase_plan()
PARTNERS = sum(len(entry[3]) for entry in PLAN)


def kernel(
    list_ref, sig_hbm, row_hbm, tr_hbm, col_hbm, near_hbm, out_hbm,
    sig, row, tr, col, near, window, mats, far_tr, far_mats, basis, send_buf, recv_buf,
    products, field, rim, out, load_sem, push_sem, pull_sem, store_sem,
):
    leaf = lax.axis_index("leaf")
    sub = lax.axis_index("sub")
    leaves = lax.axis_size("leaf")
    subs = lax.axis_size("sub")

    loads = [
        pltpu.make_async_copy(sig_hbm, sig, load_sem.at[0]),
        pltpu.make_async_copy(row_hbm, row, load_sem.at[1]),
        pltpu.make_async_copy(tr_hbm.at[:, :LOCAL], tr.at[:, :LOCAL], load_sem.at[2]),
        pltpu.make_async_copy(tr_hbm.at[:, LOCAL:], tr.at[:, LOCAL:], load_sem.at[3]),
        pltpu.make_async_copy(near_hbm, near, load_sem.at[4]),
        pltpu.make_async_copy(col_hbm, col, load_sem.at[5]),
    ]
    for load in loads:
        load.start()

    def partner(axis, bits):
        place = leaf if axis == "leaf" else sub
        for bit in bits:
            place = flipped(place, bit)
        return (place, sub) if axis == "leaf" else (leaf, place)

    rank = leaf * subs + sub
    after = (rank + 1) % (leaves * subs)
    before = (rank + leaves * subs - 1) % (leaves * subs)
    after = (after // subs, after % subs)
    before = (before // subs, before % subs)

    peers = [partner(axis, bits) for axis, _, _, sets, _ in PLAN for bits in sets]
    peers += [after, before]
    barrier = pltpu.get_barrier_semaphore()
    for peer in peers:
        pl.semaphore_signal(barrier, inc=1, device_id=peer, device_id_type=MESH)

    lane = lax.broadcasted_iota(jnp.int32, (32, LEAF), 1)
    group = lane // 32
    odd = (group % 2).astype(F32)
    upper = (group // 2).astype(F32)
    odd_b = odd.astype(BF)
    even_b = (1.0 - odd).astype(BF)
    sign_b = (1.0 - 2.0 * odd).astype(BF)
    upper_b = upper.astype(BF)
    lower_b = (1.0 - upper).astype(BF)
    first_half = lax.broadcasted_iota(jnp.int32, (RHS, LEAF), 1) < 64

    def turned(weights):
        signed = weights * sign_b
        crossed = pltpu.roll(weights, 96, 1) * even_b + pltpu.roll(weights, 32, 1) * odd_b
        return signed, crossed, pltpu.roll(signed, 64, 1), pltpu.roll(crossed, 64, 1)

    def expand(source, target):
        def body(pair, carry):
            s0, c0, sr0, cr0 = turned(source(2 * pair))
            s1, c1, sr1, cr1 = turned(source(2 * pair + 1))
            target[pair, 0] = jnp.concatenate(
                [s0 * lower_b, c0 * lower_b, sr1 * upper_b, cr1 * upper_b], axis=0
            )
            target[pair, 1] = jnp.concatenate(
                [sr0 * lower_b, cr0 * lower_b, s1 * upper_b, c1 * upper_b], axis=0
            )
            return carry

        lax.fori_loop(0, PAIRS, body, 0)

    def expand_first(source, target):
        def body(pair, carry):
            s0, c0, sr0, cr0 = turned(source(2 * pair))
            s1, c1, sr1, cr1 = turned(source(2 * pair + 1))
            target[pair, 0] = jnp.concatenate(
                [
                    s0 * lower_b + sr1 * upper_b,
                    c0 * lower_b + cr1 * upper_b,
                    sr0 * lower_b + s1 * upper_b,
                    cr0 * lower_b + c1 * upper_b,
                ],
                axis=0,
            )
            return carry

        lax.fori_loop(0, PAIRS, body, 0)

    def expand_level(level):
        expand(lambda box: tr[box, level], mats.at[level])

    loads[0].wait()
    loads[1].wait()
    coeffs = []
    for pair in range(PAIRS):
        left, right = [], []
        for box in (2 * pair, 2 * pair + 1):
            points = slice(box * LEAF, (box + 1) * LEAF)
            samples = sig[:, points]
            window[2 * REACH + box] = samples
            left.append(jnp.concatenate([samples[:RHS], samples[RHS:]], axis=1))
            real, imag = row[:32, points], row[32:, points]
            right.append(
                jnp.concatenate(
                    [jnp.concatenate([real, imag], axis=1), jnp.concatenate([-imag, real], axis=1)],
                    axis=0,
                )
            )
        product = lax.dot_general(
            jnp.concatenate(left, axis=0), jnp.concatenate(right, axis=0),
            (((1,), (1,)), ((), ())), preferred_element_type=F32,
        )
        coeffs.append(jnp.where(first_half, product[:RHS], product[RHS:]))

    loads[2].wait()
    expand_first(lambda box: tr[box, 0], mats.at[0])
    for level in range(1, LOCAL):
        expand_level(level)
    loads[3].wait()
    pl.semaphore_wait(barrier, len(peers))

    pushes = []

    def remote(source, target, number, peer):
        return pltpu.make_async_remote_copy(
            src_ref=source, dst_ref=target, send_sem=push_sem.at[number],
            recv_sem=pull_sem.at[number], device_id=peer, device_id_type=MESH,
        )

    weight_copies = {}
    for axis, bits, level, sets, slot in PLAN:
        if slot is not None:
            copy = remote(tr.at[:, level], far_tr.at[slot], PARTNERS + slot, partner(axis, sets[0]))
            copy.start()
            pushes.append(copy)
            weight_copies[slot] = copy

    coeffs = [folded(dot(pieces(coeffs[pair]), mats[0, pair, 0])) for pair in range(PAIRS)]
    for level in range(1, LOCAL):
        span = 1 << (level - 1)
        split = [pieces(values) for values in coeffs]
        following = []
        for pair in range(PAIRS):
            low = pair & ~span
            joined = jnp.concatenate([split[low], split[low | span]], axis=1)
            weights = mats[level, pair].reshape(2 * LEAF, LEAF)
            following.append(folded(dot(joined, weights)))
        coeffs = following

    edge = 2 * REACH
    halo = (
        remote(window.at[BOXES : BOXES + edge], window.at[:edge], PARTNERS + MERGED, after),
        remote(window.at[edge : 2 * edge], window.at[edge + BOXES :], PARTNERS + MERGED + 1, before),
    )

    def send_halo():
        for copy in halo:
            copy.start()
            pushes.append(copy)

    def near_field():
        for copy in halo:
            copy.wait_recv()
        loads[4].wait()

        def multiply(slot, carry):
            picked = window[jnp.maximum(list_ref[slot, 0], 0)]
            product = dot(picked, near[slot])
            real = product[:RHS, :LEAF] + product[RHS:, LEAF:]
            imag = product[RHS:, :LEAF] - product[:RHS, LEAF:]
            products[slot] = jnp.concatenate([real, imag], axis=0)
            return carry

        lax.fori_loop(0, CAP, multiply, 0)

        def gather(box, carry):
            total = jnp.zeros((2 * RHS, LEAF), F32)
            for slot in range(CAP):
                here = jnp.where(list_ref[slot, 1] == box, 1.0, 0.0).astype(F32)
                total += products[slot] * here
            field[box] = total
            return carry

        lax.fori_loop(0, BOXES + 2 * REACH, gather, 0)

    rims = (
        remote(field.at[:REACH], rim.at[0], PARTNERS + MERGED + 2, before),
        remote(field.at[BOXES + REACH :], rim.at[1], PARTNERS + MERGED + 3, after),
    )

    def send_rims():
        for copy in rims:
            copy.start()
            pushes.append(copy)

    def expand_basis():
        loads[5].wait()
        for box in range(BOXES):
            points = slice(box * LEAF, (box + 1) * LEAF)
            real, imag = col[:32, points], col[32:, points]
            basis[box // 2, 64 * (box % 2) : 64 * (box % 2) + 64] = jnp.concatenate(
                [jnp.concatenate([real, imag], axis=1), jnp.concatenate([-imag, real], axis=1)],
                axis=0,
            )

    def expand_far(slot):
        weight_copies[slot].wait_recv()
        expand(lambda box: far_tr[slot, box], far_mats.at[slot])

    fillers = [
        [lambda: expand_level(4), lambda: expand_level(5), lambda: expand_level(6),
         lambda: expand_level(7)],
        [],
        [lambda: expand_level(8), lambda: expand_level(9), near_field, send_rims],
        [lambda: expand_far(1), lambda: expand_level(10), lambda: expand_level(11),
         lambda: expand_level(12), expand_basis],
        [lambda: expand_far(2)],
        [],
    ]

    number = 0
    for step, (axis, bits, level, sets, slot) in enumerate(PLAN):
        place = leaf if axis == "leaf" else sub
        for pair in range(PAIRS):
            send_buf[step, RHS * pair : RHS * (pair + 1)] = coeffs[pair]
        copies = []
        for partner_bits in sets:
            copy = remote(
                send_buf.at[step], recv_buf.at[number], number, partner(axis, partner_bits)
            )
            copy.start()
            copies.append(copy)
            number += 1
        pushes.extend(copies)
        if step == 0:
            send_halo()
            for level_now in (4, 5):
                expand_level(level_now)
            fill = [lambda: expand_level(6), lambda: expand_level(7), lambda: expand_far(0)]
        else:
            fill = fillers[step]
        mine = bit_of(place, bits[0])
        other = 1 - mine
        partial = [
            folded(dot(pieces(coeffs[pair]), mats[level, pair, mine])) for pair in range(PAIRS)
        ]
        for task in fill:
            task()
        first = number - len(sets)

        def block(index, pair):
            return recv_buf[index, RHS * pair : RHS * (pair + 1)]

        copies[-1].wait_recv()
        coeffs = [
            partial[pair]
            + folded(dot(pieces(block(number - 1, pair)), mats[level, pair, other]))
            for pair in range(PAIRS)
        ]
        if len(bits) == 2:
            copies[0].wait_recv()
            far = [
                folded(dot(pieces(block(first, pair)), far_mats[slot, pair, mine]))
                for pair in range(PAIRS)
            ]
            mine_next = bit_of(place, bits[1])
            partial = [
                folded(dot(pieces(coeffs[pair]), mats[level + 1, pair, mine_next]))
                for pair in range(PAIRS)
            ]
            copies[1].wait_recv()
            far = [
                far[pair]
                + folded(dot(pieces(block(first + 1, pair)), far_mats[slot, pair, other]))
                for pair in range(PAIRS)
            ]
            coeffs = [
                partial[pair]
                + folded(dot(pieces(far[pair]), mats[level + 1, pair, 1 - mine_next]))
                for pair in range(PAIRS)
            ]

    for copy in rims:
        copy.wait_recv()
    for place in range(REACH):
        field[REACH + place] += rim[1, place]
        field[BOXES + place] += rim[0, place]

    stores = []
    for pair in range(PAIRS):
        values = coeffs[pair]
        zero = jnp.zeros_like(values)
        left = jnp.concatenate(
            [pieces(jnp.where(first_half, values, zero)), pieces(jnp.where(first_half, zero, values))],
            axis=0,
        )
        product = dot(left, basis[pair])
        for half in range(2):
            far_box = folded(product[2 * RHS * half : 2 * RHS * (half + 1)])
            box = 2 * pair + half
            points = slice(box * LEAF, (box + 1) * LEAF)
            near_box = field[REACH + box]
            out[:RHS, points] = far_box[:, :LEAF] + near_box[:RHS]
            out[RHS:, points] = far_box[:, LEAF:] + near_box[RHS:]
        points = slice(2 * pair * LEAF, (2 * pair + 2) * LEAF)
        store = pltpu.make_async_copy(out.at[:, points], out_hbm.at[:, points], store_sem.at[pair])
        store.start()
        stores.append(store)
    for copy in pushes:
        copy.wait_send()
    for store in stores:
        store.wait()


def shards(signal, row_basis, transfer, column_basis, near_blocks, near_list):
    anywhere = pl.BlockSpec(memory_space=pl.ANY)
    copies = PARTNERS + MERGED + 4
    return pl.pallas_call(
        kernel,
        out_shape=jax.ShapeDtypeStruct((2 * RHS, BOXES * LEAF), F32),
        in_specs=[pl.BlockSpec(memory_space=pltpu.SMEM)] + [anywhere] * 5,
        out_specs=anywhere,
        scratch_shapes=[
            pltpu.VMEM((2 * RHS, BOXES * LEAF), BF),
            pltpu.VMEM((64, BOXES * LEAF), BF),
            pltpu.VMEM((BOXES, LEVELS, 32, LEAF), BF),
            pltpu.VMEM((64, BOXES * LEAF), BF),
            pltpu.VMEM((CAP, LEAF, 2 * LEAF), BF),
            pltpu.VMEM((BOXES + 4 * REACH, 2 * RHS, LEAF), BF),
            pltpu.VMEM((LEVELS, PAIRS, 2, LEAF, LEAF), BF),
            pltpu.VMEM((MERGED, BOXES, 32, LEAF), BF),
            pltpu.VMEM((MERGED, PAIRS, 2, LEAF, LEAF), BF),
            pltpu.VMEM((PAIRS, LEAF, 2 * LEAF), BF),
            pltpu.VMEM((len(PLAN), PAIRS * RHS, LEAF), F32),
            pltpu.VMEM((PARTNERS, PAIRS * RHS, LEAF), F32),
            pltpu.VMEM((CAP, 2 * RHS, LEAF), F32),
            pltpu.VMEM((BOXES + 2 * REACH, 2 * RHS, LEAF), F32),
            pltpu.VMEM((2, REACH, 2 * RHS, LEAF), F32),
            pltpu.VMEM((2 * RHS, BOXES * LEAF), F32),
            pltpu.SemaphoreType.DMA((6,)),
            pltpu.SemaphoreType.DMA((copies,)),
            pltpu.SemaphoreType.DMA((copies,)),
            pltpu.SemaphoreType.DMA((PAIRS,)),
        ],
        compiler_params=pltpu.CompilerParams(
            collective_id=0, has_side_effects=True, vmem_limit_bytes=56 * 1024 * 1024
        ),
        name="adjoint",
    )(near_list, signal, row_basis, transfer, column_basis, near_blocks)


def solution(mesh):
    return jax.shard_map(
        shards,
        mesh=mesh,
        in_specs=(
            P(None, ("leaf", "sub")),
            P(None, ("leaf", "sub")),
            P(("leaf", "sub"), None, None, None),
            P(None, ("leaf", "sub")),
            P(("leaf", "sub"), None, None),
            P(("leaf", "sub"), None),
        ),
        out_specs=P(None, ("leaf", "sub")),
        check_vma=False,
    )
```

```python
import functools

import jax
import jax.numpy as jnp
from jax import lax
from jax.experimental import pallas as pl
from jax.experimental.pallas import tpu as pltpu
from jax.sharding import PartitionSpec as P

LEAF = 128
BOXES = 16
PAIRS = 8
RHS = 16
CAP = 24
REACH = 4
LEVELS = 13
LOCAL = 4
PHASES = (
    ("sub", (0, 1)),
    ("leaf", (0,)),
    ("leaf", (1,)),
    ("leaf", (2, 3)),
    ("leaf", (4,)),
    ("leaf", (5, 6)),
)
FULL = 32767.0
SMALLEST = 1e-30

BF = jnp.bfloat16
F32 = jnp.float32
MESH = pl.DeviceIdType.MESH


def bit_of(index, bit):
    return (index // (1 << bit)) % 2


def flipped(index, bit):
    return index + (1 - 2 * bit_of(index, bit)) * (1 << bit)


def pieces(values):
    high = values.astype(BF)
    low = (values - high.astype(F32)).astype(BF)
    return jnp.concatenate([high, low], axis=0)


def folded(product):
    half = product.shape[0] // 2
    return product[:half] + product[half:]


def dot(left, right):
    return jnp.dot(left, right, preferred_element_type=F32)


def coded(coeffs):
    peak = jnp.abs(coeffs[0])
    for values in coeffs[1:]:
        peak = jnp.maximum(peak, jnp.abs(values))
    peak = jnp.maximum(jnp.maximum(peak[:8], peak[8:]), SMALLEST)
    inverse = FULL / peak
    inverse = jnp.concatenate([inverse, inverse], axis=0)
    codes = [jnp.round(values * inverse).astype(jnp.int32).astype(jnp.int16) for values in coeffs]
    return codes, peak * (1.0 / FULL)


def phase_plan():
    plan = []
    level = LOCAL
    slot = 0
    for axis, bits in PHASES:
        if len(bits) == 1:
            plan.append((axis, bits, level, ((bits[0],),), None))
        else:
            low, high = bits
            plan.append((axis, bits, level, ((high,), (low, high), (low,)), slot))
            slot += 1
        level += len(bits)
    return tuple(plan), slot


PLAN, MERGED = phase_plan()
PARTNERS = sum(len(entry[3]) for entry in PLAN)
SCALES = PARTNERS + MERGED + 4


def kernel(
    list_ref, sig_hbm, row_hbm, tr_hbm, col_hbm, near_hbm, out,
    sig, row, tr, col, near, window, mats, far_tr, far_mats, basis, send_buf, recv_buf, send_scale, recv_scale,
    products, field, rim, load_sem, push_sem, pull_sem,
):
    leaf = lax.axis_index("leaf")
    sub = lax.axis_index("sub")
    leaves = lax.axis_size("leaf")
    subs = lax.axis_size("sub")

    loads = [
        pltpu.make_async_copy(sig_hbm, sig, load_sem.at[0]),
        pltpu.make_async_copy(row_hbm, row, load_sem.at[1]),
        pltpu.make_async_copy(tr_hbm.at[:, :LOCAL], tr.at[:, :LOCAL], load_sem.at[2]),
        pltpu.make_async_copy(tr_hbm.at[:, LOCAL:], tr.at[:, LOCAL:], load_sem.at[3]),
        pltpu.make_async_copy(near_hbm, near, load_sem.at[4]),
        pltpu.make_async_copy(col_hbm, col, load_sem.at[5]),
    ]
    for load in loads:
        load.start()

    def partner(axis, bits):
        place = leaf if axis == "leaf" else sub
        for bit in bits:
            place = flipped(place, bit)
        return (place, sub) if axis == "leaf" else (leaf, place)

    rank = leaf * subs + sub
    after = (rank + 1) % (leaves * subs)
    before = (rank + leaves * subs - 1) % (leaves * subs)
    after = (after // subs, after % subs)
    before = (before // subs, before % subs)

    peers = [partner(axis, bits) for axis, _, _, sets, _ in PLAN for bits in sets]
    peers += [after, before]
    barrier = pltpu.get_barrier_semaphore()
    for peer in peers:
        pl.semaphore_signal(barrier, inc=1, device_id=peer, device_id_type=MESH)

    lane = lax.broadcasted_iota(jnp.int32, (32, LEAF), 1)
    group = lane // 32
    odd = (group % 2).astype(F32)
    upper = (group // 2).astype(F32)
    odd_b = odd.astype(BF)
    even_b = (1.0 - odd).astype(BF)
    sign_b = (1.0 - 2.0 * odd).astype(BF)
    upper_b = upper.astype(BF)
    lower_b = (1.0 - upper).astype(BF)
    first_half = lax.broadcasted_iota(jnp.int32, (RHS, LEAF), 1) < 64

    def turned(weights):
        by32, by64, by96 = (pltpu.roll(weights, shift, 1) for shift in (32, 64, 96))
        return (
            weights * sign_b,
            by96 * even_b + by32 * odd_b,
            by64 * sign_b,
            by32 * even_b + by96 * odd_b,
        )

    def expand(source, target):
        def body(pair, carry):
            s0, c0, sr0, cr0 = turned(source(2 * pair))
            s1, c1, sr1, cr1 = turned(source(2 * pair + 1))
            target[pair, 0] = jnp.concatenate(
                [s0 * lower_b, c0 * lower_b, sr1 * upper_b, cr1 * upper_b], axis=0
            )
            target[pair, 1] = jnp.concatenate(
                [sr0 * lower_b, cr0 * lower_b, s1 * upper_b, c1 * upper_b], axis=0
            )
            return carry

        lax.fori_loop(0, PAIRS, body, 0, unroll=8)

    def expand_first(source, target):
        def body(pair, carry):
            s0, c0, sr0, cr0 = turned(source(2 * pair))
            s1, c1, sr1, cr1 = turned(source(2 * pair + 1))
            target[pair, 0] = jnp.concatenate(
                [
                    s0 * lower_b + sr1 * upper_b,
                    c0 * lower_b + cr1 * upper_b,
                    sr0 * lower_b + s1 * upper_b,
                    cr0 * lower_b + c1 * upper_b,
                ],
                axis=0,
            )
            return carry

        lax.fori_loop(0, PAIRS, body, 0, unroll=8)

    def expand_level(level):
        expand(lambda box: tr[box, level], mats.at[level])

    loads[0].wait()
    loads[1].wait()
    coeffs = []
    for pair in range(PAIRS):
        left, right = [], []
        for box in (2 * pair, 2 * pair + 1):
            points = slice(box * LEAF, (box + 1) * LEAF)
            samples = sig[:, points]
            window[2 * REACH + box] = samples
            left.append(jnp.concatenate([samples[:RHS], samples[RHS:]], axis=1))
            real, imag = row[:32, points], row[32:, points]
            right.append(
                jnp.concatenate(
                    [jnp.concatenate([real, imag], axis=1), jnp.concatenate([-imag, real], axis=1)],
                    axis=0,
                )
            )
        product = lax.dot_general(
            jnp.concatenate(left, axis=0), jnp.concatenate(right, axis=0),
            (((1,), (1,)), ((), ())), preferred_element_type=F32,
        )
        coeffs.append(jnp.where(first_half, product[:RHS], product[RHS:]))

    loads[2].wait()
    expand_first(lambda box: tr[box, 0], mats.at[0])
    for level in range(1, LOCAL):
        expand_level(level)
    loads[3].wait()
    pl.semaphore_wait(barrier, len(peers))

    pushes = []

    def remote(source, target, number, peer):
        return pltpu.make_async_remote_copy(
            src_ref=source, dst_ref=target, send_sem=push_sem.at[number],
            recv_sem=pull_sem.at[number], device_id=peer, device_id_type=MESH,
        )

    weight_copies = {}
    for axis, bits, level, sets, slot in PLAN:
        if slot is not None:
            copy = remote(tr.at[:, level], far_tr.at[slot], PARTNERS + slot, partner(axis, sets[0]))
            copy.start()
            pushes.append(copy)
            weight_copies[slot] = copy

    coeffs = [folded(dot(pieces(coeffs[pair]), mats[0, pair, 0])) for pair in range(PAIRS)]
    for level in range(1, LOCAL):
        span = 1 << (level - 1)
        split = [pieces(values) for values in coeffs]
        following = []
        for pair in range(PAIRS):
            low = pair & ~span
            joined = jnp.concatenate([split[low], split[low | span]], axis=1)
            weights = mats[level, pair].reshape(2 * LEAF, LEAF)
            following.append(folded(dot(joined, weights)))
        coeffs = following

    edge = 2 * REACH
    halo = (
        remote(window.at[BOXES : BOXES + edge], window.at[:edge], PARTNERS + MERGED, after),
        remote(window.at[edge : 2 * edge], window.at[edge + BOXES :], PARTNERS + MERGED + 1, before),
    )

    def send_halo():
        for copy in halo:
            copy.start()
            pushes.append(copy)

    def near_field():
        for copy in halo:
            copy.wait_recv()
        loads[4].wait()

        def multiply(slot, carry):
            picked = window[jnp.maximum(list_ref[0, slot], 0)]
            product = dot(picked, near[slot])
            real = product[:RHS, :LEAF] + product[RHS:, LEAF:]
            imag = product[RHS:, :LEAF] - product[:RHS, LEAF:]
            products[slot] = jnp.concatenate([real, imag], axis=0)
            return carry

        lax.fori_loop(0, CAP, multiply, 0, unroll=8)

        def gather(box, carry):
            total = jnp.zeros((2 * RHS, LEAF), F32)
            for slot in range(CAP):
                here = jnp.where(list_ref[1, slot] == box, 1.0, 0.0).astype(F32)
                total += products[slot] * here
            field[box] = total
            return carry

        lax.fori_loop(0, BOXES + 2 * REACH, gather, 0)

    rims = (
        remote(field.at[:REACH], rim.at[0], PARTNERS + MERGED + 2, before),
        remote(field.at[BOXES + REACH :], rim.at[1], PARTNERS + MERGED + 3, after),
    )

    def send_rims():
        for copy in rims:
            copy.start()
            pushes.append(copy)

    def expand_basis():
        loads[5].wait()
        for box in range(BOXES):
            points = slice(box * LEAF, (box + 1) * LEAF)
            real, imag = col[:32, points], col[32:, points]
            basis[box // 2, 64 * (box % 2) : 64 * (box % 2) + 64] = jnp.concatenate(
                [jnp.concatenate([real, imag], axis=1), jnp.concatenate([-imag, real], axis=1)],
                axis=0,
            )

    def expand_far(slot):
        weight_copies[slot].wait_recv()
        expand(lambda box: far_tr[slot, box], far_mats.at[slot])

    fillers = [
        [lambda: expand_level(4), lambda: expand_level(5), lambda: expand_level(6),
         lambda: expand_level(7)],
        [],
        [lambda: expand_level(8), lambda: expand_level(9), near_field, send_rims],
        [lambda: expand_far(1), lambda: expand_level(10), lambda: expand_level(11),
         lambda: expand_level(12), expand_basis],
        [lambda: expand_far(2)],
        [],
    ]

    number = 0
    for step, (axis, bits, level, sets, slot) in enumerate(PLAN):
        place = leaf if axis == "leaf" else sub
        codes, scale = coded(coeffs)
        for pair in range(PAIRS):
            send_buf[step, RHS * pair : RHS * (pair + 1)] = codes[pair]
        send_scale[step] = scale
        copies = []
        for partner_bits in sets:
            peer = partner(axis, partner_bits)
            both = (
                remote(send_scale.at[step], recv_scale.at[number], SCALES + number, peer),
                remote(send_buf.at[step], recv_buf.at[number], number, peer),
            )
            for copy in both:
                copy.start()
            pushes.extend(both)
            copies.append(both)
            number += 1
        if step == 0:
            send_halo()
            for level_now in (4, 5):
                expand_level(level_now)
            fill = [lambda: expand_level(6), lambda: expand_level(7), lambda: expand_far(0)]
        else:
            fill = fillers[step]
        mine = bit_of(place, bits[0])
        other = 1 - mine
        partial = [
            folded(dot(pieces(coeffs[pair]), mats[level, pair, mine])) for pair in range(PAIRS)
        ]
        for task in fill:
            task()
        first = number - len(sets)

        def block(index, pair):
            scale = recv_scale[index]
            scale = jnp.concatenate([scale, scale], axis=0)
            return recv_buf[index, RHS * pair : RHS * (pair + 1)].astype(F32) * scale

        def arrived(both):
            for copy in both:
                copy.wait_recv()

        arrived(copies[-1])
        coeffs = [
            partial[pair]
            + folded(dot(pieces(block(number - 1, pair)), mats[level, pair, other]))
            for pair in range(PAIRS)
        ]
        if len(bits) == 2:
            arrived(copies[0])
            far = [
                folded(dot(pieces(block(first, pair)), far_mats[slot, pair, mine]))
                for pair in range(PAIRS)
            ]
            mine_next = bit_of(place, bits[1])
            partial = [
                folded(dot(pieces(coeffs[pair]), mats[level + 1, pair, mine_next]))
                for pair in range(PAIRS)
            ]
            arrived(copies[1])
            far = [
                far[pair]
                + folded(dot(pieces(block(first + 1, pair)), far_mats[slot, pair, other]))
                for pair in range(PAIRS)
            ]
            coeffs = [
                partial[pair]
                + folded(dot(pieces(far[pair]), mats[level + 1, pair, 1 - mine_next]))
                for pair in range(PAIRS)
            ]

    for copy in rims:
        copy.wait_recv()
    for place in range(REACH):
        field[REACH + place] += rim[1, place]
        field[BOXES + place] += rim[0, place]

    for pair in range(PAIRS):
        values = coeffs[pair]
        zero = jnp.zeros_like(values)
        left = jnp.concatenate(
            [pieces(jnp.where(first_half, values, zero)), pieces(jnp.where(first_half, zero, values))],
            axis=0,
        )
        product = dot(left, basis[pair])
        for half in range(2):
            far_box = folded(product[2 * RHS * half : 2 * RHS * (half + 1)])
            box = 2 * pair + half
            points = slice(box * LEAF, (box + 1) * LEAF)
            near_box = field[REACH + box]
            out[:RHS, points] = far_box[:, :LEAF] + near_box[:RHS]
            out[RHS:, points] = far_box[:, LEAF:] + near_box[RHS:]
    for copy in pushes:
        copy.wait_send()


def shards(signal, row_basis, transfer, column_basis, near_blocks, near_list):
    anywhere = pl.BlockSpec(memory_space=pl.ANY)
    copies = SCALES + PARTNERS
    return pl.pallas_call(
        kernel,
        out_shape=jax.ShapeDtypeStruct((2 * RHS, BOXES * LEAF), F32),
        in_specs=[pl.BlockSpec(memory_space=pltpu.SMEM)] + [anywhere] * 5,
        out_specs=pl.BlockSpec(memory_space=pltpu.VMEM),
        scratch_shapes=[
            pltpu.VMEM((2 * RHS, BOXES * LEAF), BF),
            pltpu.VMEM((64, BOXES * LEAF), BF),
            pltpu.VMEM((BOXES, LEVELS, 32, LEAF), BF),
            pltpu.VMEM((64, BOXES * LEAF), BF),
            pltpu.VMEM((CAP, LEAF, 2 * LEAF), BF),
            pltpu.VMEM((BOXES + 4 * REACH, 2 * RHS, LEAF), BF),
            pltpu.VMEM((LEVELS, PAIRS, 2, LEAF, LEAF), BF),
            pltpu.VMEM((MERGED, BOXES, 32, LEAF), BF),
            pltpu.VMEM((MERGED, PAIRS, 2, LEAF, LEAF), BF),
            pltpu.VMEM((PAIRS, LEAF, 2 * LEAF), BF),
            pltpu.VMEM((len(PLAN), PAIRS * RHS, LEAF), jnp.int16),
            pltpu.VMEM((PARTNERS, PAIRS * RHS, LEAF), jnp.int16),
            pltpu.VMEM((len(PLAN), 8, LEAF), F32),
            pltpu.VMEM((PARTNERS, 8, LEAF), F32),
            pltpu.VMEM((CAP, 2 * RHS, LEAF), F32),
            pltpu.VMEM((BOXES + 2 * REACH, 2 * RHS, LEAF), F32),
            pltpu.VMEM((2, REACH, 2 * RHS, LEAF), F32),
            pltpu.SemaphoreType.DMA((6,)),
            pltpu.SemaphoreType.DMA((copies,)),
            pltpu.SemaphoreType.DMA((copies,)),
        ],
        compiler_params=pltpu.CompilerParams(
            collective_id=0, has_side_effects=True, vmem_limit_bytes=56 * 1024 * 1024
        ),
        name="adjoint",
    )(near_list.T, signal, row_basis, transfer, column_basis, near_blocks)


def solution(mesh):
    return jax.shard_map(
        shards,
        mesh=mesh,
        in_specs=(
            P(None, ("leaf", "sub")),
            P(None, ("leaf", "sub")),
            P(("leaf", "sub"), None, None, None),
            P(None, ("leaf", "sub")),
            P(("leaf", "sub"), None, None),
            P(("leaf", "sub"), None),
        ),
        out_specs=P(None, ("leaf", "sub")),
        check_vma=False,
    )
```

```python
import functools

import jax
import jax.numpy as jnp
from jax import lax
from jax.experimental import pallas as pl
from jax.experimental.pallas import tpu as pltpu
from jax.sharding import PartitionSpec as P

LEAF = 128
BOXES = 16
PAIRS = 8
RHS = 16
CAP = 24
REACH = 4
LEVELS = 13
LOCAL = 4
GROUPS = 1
WIDTH = PAIRS // GROUPS
PHASES = (
    ((("sub", 0), ("sub", 1)), "receive"),
    ((("leaf", 0), ("leaf", 1)), "send"),
    ((("leaf", 2), ("leaf", 3)), "send"),
    ((("leaf", 4),), "one"),
    ((("leaf", 5), ("leaf", 6)), "send"),
)
FULL = 32767.0
SMALLEST = 1e-30

BF = jnp.bfloat16
F32 = jnp.float32
MESH = pl.DeviceIdType.MESH


def bit_of(index, bit):
    return (index // (1 << bit)) % 2


def flipped(index, bit):
    return index + (1 - 2 * bit_of(index, bit)) * (1 << bit)


def pieces(values):
    high = values.astype(BF)
    low = (values - high.astype(F32)).astype(BF)
    return jnp.concatenate([high, low], axis=0)


def folded(product):
    half = product.shape[0] // 2
    return product[:half] + product[half:]


def dot(left, right):
    return jnp.dot(left, right, preferred_element_type=F32)


def coded(coeffs):
    peak = jnp.abs(coeffs[0])
    for values in coeffs[1:]:
        peak = jnp.maximum(peak, jnp.abs(values))
    peak = jnp.maximum(jnp.maximum(peak[:8], peak[8:]), SMALLEST)
    inverse = FULL / peak
    inverse = jnp.concatenate([inverse, inverse], axis=0)
    codes = [jnp.round(values * inverse).astype(jnp.int32).astype(jnp.int16) for values in coeffs]
    return codes, peak * (1.0 / FULL)


def phase_plan():
    plan = []
    level = LOCAL
    slot = 0
    for bits, mode in PHASES:
        if mode == "one":
            plan.append((bits, level, mode, (bits,), None))
        else:
            low, high = bits
            plan.append((bits, level, mode, ((high,), (low, high), (low,)), slot))
            slot += 1
        level += len(bits)
    return tuple(plan), slot


PLAN, MERGED = phase_plan()
PARTNERS = sum(len(entry[3]) for entry in PLAN)
WEIGHTS = PARTNERS * GROUPS
HALO = WEIGHTS + MERGED
RIM = HALO + 2
COPIES = RIM + 2
CODE_ROWS = WIDTH * RHS
SCALE_ROWS = 16
SENT_ROWS = (
    PARTNERS * GROUPS * (CODE_ROWS + SCALE_ROWS)
    + MERGED * PAIRS * 32
    + 2 * 2 * REACH * 2 * RHS
    + 2 * REACH * 2 * RHS * 2
)


def kernel(
    list_hbm, sig_hbm, row_hbm, tr_hbm, col_hbm, near_hbm, out,
    sig, row, tr, col, near, window, mats, packed, far_tr, far_mats, basis, send_buf, recv_buf, send_scale, recv_scale,
    products, field, rim, list_ref, tally, load_sem, push_sem, pull_sem,
):
    leaf = lax.axis_index("leaf")
    sub = lax.axis_index("sub")
    leaves = lax.axis_size("leaf")
    subs = lax.axis_size("sub")

    loads = [
        pltpu.make_async_copy(sig_hbm, sig, load_sem.at[0]),
        pltpu.make_async_copy(row_hbm, row, load_sem.at[1]),
        pltpu.make_async_copy(tr_hbm.at[:, : LOCAL + 1], tr.at[:, : LOCAL + 1], load_sem.at[2]),
        pltpu.make_async_copy(tr_hbm.at[:, LOCAL + 1 :], tr.at[:, LOCAL + 1 :], load_sem.at[3]),
        pltpu.make_async_copy(near_hbm, near, load_sem.at[4]),
        pltpu.make_async_copy(col_hbm, col, load_sem.at[5]),
        pltpu.make_async_copy(list_hbm, list_ref, load_sem.at[6]),
    ]
    for load in loads:
        load.start()

    def partner(bits):
        places = {"leaf": leaf, "sub": sub}
        for axis, bit in bits:
            places[axis] = flipped(places[axis], bit)
        return places["leaf"], places["sub"]

    def side(step, which):
        axis, bit = PLAN[step][0][which]
        return bit_of(leaf if axis == "leaf" else sub, bit)

    rank = leaf * subs + sub
    after = (rank + 1) % (leaves * subs)
    before = (rank + leaves * subs - 1) % (leaves * subs)
    after = (after // subs, after % subs)
    before = (before // subs, before % subs)

    peers = [partner(bits) for entry in PLAN for bits in entry[3]]
    peers += [after, before]
    barrier = pltpu.get_barrier_semaphore()
    for peer in peers:
        pl.semaphore_signal(barrier, inc=1, device_id=peer, device_id_type=MESH)

    lane = lax.broadcasted_iota(jnp.int32, (32, LEAF), 1)
    group = lane // 32
    odd = (group % 2).astype(F32)
    upper = (group // 2).astype(F32)
    odd_b = odd.astype(BF)
    even_b = (1.0 - odd).astype(BF)
    sign_b = (1.0 - 2.0 * odd).astype(BF)
    upper_b = upper.astype(BF)
    lower_b = (1.0 - upper).astype(BF)
    first_half = lax.broadcasted_iota(jnp.int32, (RHS, LEAF), 1) < 64

    def turned(weights):
        by32, by64, by96 = (pltpu.roll(weights, shift, 1) for shift in (32, 64, 96))
        return (
            weights * sign_b,
            by96 * even_b + by32 * odd_b,
            by64 * sign_b,
            by32 * even_b + by96 * odd_b,
        )

    def expand(source, target, pairs=(0, PAIRS)):
        def body(pair, carry):
            s0, c0, sr0, cr0 = turned(source(2 * pair))
            s1, c1, sr1, cr1 = turned(source(2 * pair + 1))
            target[pair, 0] = jnp.concatenate(
                [s0 * lower_b, c0 * lower_b, sr1 * upper_b, cr1 * upper_b], axis=0
            )
            target[pair, 1] = jnp.concatenate(
                [sr0 * lower_b, cr0 * lower_b, s1 * upper_b, c1 * upper_b], axis=0
            )
            return carry

        lax.fori_loop(*pairs, body, 0, unroll=8)

    def expand_first(source, target):
        def body(pair, carry):
            s0, c0, sr0, cr0 = turned(source(2 * pair))
            s1, c1, sr1, cr1 = turned(source(2 * pair + 1))
            target[pair, 0] = jnp.concatenate(
                [
                    s0 * lower_b + sr1 * upper_b,
                    c0 * lower_b + cr1 * upper_b,
                    sr0 * lower_b + s1 * upper_b,
                    cr0 * lower_b + c1 * upper_b,
                ],
                axis=0,
            )
            return carry

        lax.fori_loop(0, PAIRS, body, 0, unroll=8)

    def expand_level(level):
        expand(lambda box: tr[box, level], mats.at[level])

    for load in loads[:3]:
        load.wait()
    def remote(source, target, number, peer):
        return pltpu.make_async_remote_copy(
            src_ref=source, dst_ref=target, send_sem=push_sem,
            recv_sem=pull_sem.at[number], device_id=peer, device_id_type=MESH,
        )

    weight_copies = {}
    for step, (_, _, mode, sets, slot) in enumerate(PLAN):
        if slot is not None:
            weight_copies[slot] = remote(
                packed.at[slot], far_tr.at[slot], WEIGHTS + slot,
                partner(sets[0] if mode == "receive" else sets[2]),
            )

    def pack(step):
        _, level, _, _, slot = PLAN[step]
        upper_child = (1 - side(step, 0)).astype(F32)
        straight = ((1.0 - upper) * (1.0 - upper_child)).astype(BF)
        straight_next = (upper * upper_child).astype(BF)
        turned_round = ((1.0 - upper) * upper_child).astype(BF)
        turned_next = (upper * (1.0 - upper_child)).astype(BF)
        for pair in range(PAIRS):
            one, two = tr[2 * pair, level], tr[2 * pair + 1, level]
            packed[slot, pair] = (
                one * straight
                + pltpu.roll(one, 64, 1) * turned_round
                + two * straight_next
                + pltpu.roll(two, 64, 1) * turned_next
            )

    pack(0)
    coeffs = []
    for pair in range(PAIRS):
        left, right = [], []
        for box in (2 * pair, 2 * pair + 1):
            points = slice(box * LEAF, (box + 1) * LEAF)
            samples = sig[:, points]
            window[2 * REACH + box] = samples
            left.append(jnp.concatenate([samples[:RHS], samples[RHS:]], axis=1))
            real, imag = row[:32, points], row[32:, points]
            right.append(
                jnp.concatenate(
                    [jnp.concatenate([real, imag], axis=1), jnp.concatenate([-imag, real], axis=1)],
                    axis=0,
                )
            )
        product = lax.dot_general(
            jnp.concatenate(left, axis=0), jnp.concatenate(right, axis=0),
            (((1,), (1,)), ((), ())), preferred_element_type=F32,
        )
        coeffs.append(jnp.where(first_half, product[:RHS], product[RHS:]))

    expand_first(lambda box: tr[box, 0], mats.at[0])
    for level in range(1, LOCAL):
        expand_level(level)

    pl.semaphore_wait(barrier, len(peers))
    weight_copies[0].start()

    coeffs = [folded(dot(pieces(coeffs[pair]), mats[0, pair, 0])) for pair in range(PAIRS)]
    for level in range(1, LOCAL):
        span = 1 << (level - 1)
        split = [pieces(values) for values in coeffs]
        following = []
        for pair in range(PAIRS):
            low = pair & ~span
            joined = jnp.concatenate([split[low], split[low | span]], axis=1)
            weights = mats[level, pair].reshape(2 * LEAF, LEAF)
            following.append(folded(dot(joined, weights)))
        coeffs = following

    edge = 2 * REACH
    halo = (
        remote(window.at[BOXES : BOXES + edge], window.at[:edge], HALO, after),
        remote(window.at[edge : 2 * edge], window.at[edge + BOXES :], HALO + 1, before),
    )

    def send_halo():
        for copy in halo:
            copy.start()

    def near_field():
        for copy in halo:
            copy.wait_recv()
        loads[4].wait()
        loads[6].wait()

        def multiply(slot, carry):
            picked = window[jnp.maximum(list_ref[0, slot], 0)]
            product = dot(picked, near[slot])
            real = product[:RHS, :LEAF] + product[RHS:, LEAF:]
            imag = product[RHS:, :LEAF] - product[:RHS, LEAF:]
            products[slot] = jnp.concatenate([real, imag], axis=0)
            return carry

        lax.fori_loop(0, CAP, multiply, 0, unroll=8)

        def gather(box, carry):
            total = jnp.zeros((2 * RHS, LEAF), F32)
            for slot in range(CAP):
                here = jnp.where(list_ref[1, slot] == box, 1.0, 0.0).astype(F32)
                total += products[slot] * here
            field[box] = total
            return carry

        lax.fori_loop(0, BOXES + 2 * REACH, gather, 0)

    rims = (
        remote(field.at[:REACH], rim.at[0], RIM, before),
        remote(field.at[BOXES + REACH :], rim.at[1], RIM + 1, after),
    )

    def send_rims():
        for copy in rims:
            copy.start()

    def expand_basis():
        loads[5].wait()
        for box in range(BOXES):
            points = slice(box * LEAF, (box + 1) * LEAF)
            real, imag = col[:32, points], col[32:, points]
            basis[box // 2, 64 * (box % 2) : 64 * (box % 2) + 64] = jnp.concatenate(
                [jnp.concatenate([real, imag], axis=1), jnp.concatenate([-imag, real], axis=1)],
                axis=0,
            )

    def finish_near():
        for copy in rims:
            copy.wait_recv()
        for place in range(REACH):
            field[REACH + place] += rim[1, place]
            field[BOXES + place] += rim[0, place]

    def finish(pair, values):
        zero = jnp.zeros_like(values)
        left = jnp.concatenate(
            [pieces(jnp.where(first_half, values, zero)), pieces(jnp.where(first_half, zero, values))],
            axis=0,
        )
        product = dot(left, basis[pair])
        for half in range(2):
            far_box = folded(product[2 * RHS * half : 2 * RHS * (half + 1)])
            box = 2 * pair + half
            points = slice(box * LEAF, (box + 1) * LEAF)
            near_box = field[REACH + box]
            out[:RHS, points] = far_box[:, :LEAF] + near_box[:RHS]
            out[RHS:, points] = far_box[:, LEAF:] + near_box[RHS:]

    def expand_far(slot):
        weight_copies[slot].wait_recv()
        for pair in range(PAIRS):
            weights = far_tr[slot, pair]
            signed = weights * sign_b
            crossed = pltpu.roll(weights, 96, 1) * even_b + pltpu.roll(weights, 32, 1) * odd_b
            far_mats[slot, pair] = jnp.concatenate(
                [signed * lower_b, crossed * lower_b, signed * upper_b, crossed * upper_b], axis=0
            )

    def fill(step):
        if step == 0:
            loads[3].wait()
            for later in range(1, len(PLAN)):
                if PLAN[later][4] is not None:
                    pack(later)
                    weight_copies[PLAN[later][4]].start()
            for level in range(LOCAL + 1, LEVELS):
                expand_level(level)
            expand_basis()
            expand_far(1)
            expand_far(0)
        elif step == 1:
            send_halo()
            expand_far(2)
        elif step == 2:
            expand_far(3)
            near_field()
            send_rims()

    first_number = []
    total = 0
    for entry in PLAN:
        first_number.append(total)
        total += len(entry[3])

    def number_of(step, group, order):
        return GROUPS * (first_number[step] + order) + group

    def push(step, group, which, values, orders):
        codes, scale = coded(values)
        for index, code in enumerate(codes):
            send_buf[2 * step + which, group, RHS * index : RHS * (index + 1)] = code
        send_scale[2 * step + which, group] = scale
        for order in orders:
            number = number_of(step, group, order)
            peer = partner(PLAN[step][3][order])
            remote(
                send_scale.at[2 * step + which, group], recv_scale.at[number], number, peer
            ).start()
            remote(send_buf.at[2 * step + which, group], recv_buf.at[number], number, peer).start()

    def arrived(step, group, order):
        number = number_of(step, group, order)
        both = tally.at[: CODE_ROWS + SCALE_ROWS]
        pltpu.make_async_copy(both, both, pull_sem.at[number]).wait()
        scale = recv_scale[number]
        scale = jnp.concatenate([scale, scale], axis=0)
        return [
            recv_buf[number, RHS * index : RHS * (index + 1)].astype(F32) * scale
            for index in range(WIDTH)
        ]

    def times(values, weights):
        return [folded(dot(pieces(values[index]), weights(index))) for index in range(WIDTH)]

    def sums(left, right):
        return [one + two for one, two in zip(left, right)]

    def matrices(level, group, child):
        return lambda index: mats[level, WIDTH * group + index, child]

    def send(step, group, values):
        _, level, mode, _, slot = PLAN[step]
        mine = matrices(level, group, side(step, 0))
        if mode == "one":
            push(step, group, 0, values, (0,))
            return lambda: times(values, mine)
        if mode == "receive":
            push(step, group, 0, values, (1, 2))
            if step == 0:
                expand_level(level)
            own = times(values, mine)
            push(step, group, 1, own, (0,))
            return lambda: own
        both = [
            folded(
                dot(
                    pieces(values[index]),
                    jnp.concatenate(
                        [mine(index), far_mats[slot, WIDTH * group + index]], axis=1
                    ),
                )
            )
            for index in range(WIDTH)
        ]
        own = [value[:, :LEAF] for value in both]
        push(step, group, 1, own, (0,))
        push(step, group, 0, [value[:, LEAF:] for value in both], (1, 2))
        return lambda: own

    coeffs = [coeffs[WIDTH * group : WIDTH * (group + 1)] for group in range(GROUPS)]
    partial = [send(0, group, coeffs[group])() for group in range(GROUPS)]
    for step, (bits, level, mode, sets, slot) in enumerate(PLAN):
        fill(step)
        for group in range(GROUPS):
            other = matrices(level, group, 1 - side(step, 0))
            if mode == "one":
                values = sums(partial[group], times(arrived(step, group, 0), other))
            else:
                values = arrived(step, group, 2)
                if mode == "receive":
                    values = times(values, other)
                values = sums(partial[group], values)
                mine_next = side(step, 1)
                ahead = times(values, matrices(level + 1, group, mine_next))
                far = arrived(step, group, 1)
                if mode == "receive":
                    far = times(far, lambda index: far_mats[slot, WIDTH * group + index])
                far = sums(far, arrived(step, group, 0))
                values = sums(ahead, times(far, matrices(level + 1, group, 1 - mine_next)))
            coeffs[group] = values
            if step + 1 < len(PLAN):
                partial[group] = send(step + 1, group, values)()
            else:
                if group == 0:
                    finish_near()
                for index in range(WIDTH):
                    finish(WIDTH * group + index, values[index])

    pltpu.make_async_copy(tally, tally, push_sem).wait()


def shards(signal, row_basis, transfer, column_basis, near_blocks, near_list):
    anywhere = pl.BlockSpec(memory_space=pltpu.HBM)
    return pl.pallas_call(
        kernel,
        out_shape=pltpu.VMEM((2 * RHS, BOXES * LEAF), F32),
        in_specs=[anywhere] * 6,
        out_specs=pl.BlockSpec(memory_space=pltpu.VMEM),
        scratch_shapes=[
            pltpu.VMEM((2 * RHS, BOXES * LEAF), BF),
            pltpu.VMEM((64, BOXES * LEAF), BF),
            pltpu.VMEM((BOXES, LEVELS, 32, LEAF), BF),
            pltpu.VMEM((64, BOXES * LEAF), BF),
            pltpu.VMEM((CAP, LEAF, 2 * LEAF), BF),
            pltpu.VMEM((BOXES + 4 * REACH, 2 * RHS, LEAF), BF),
            pltpu.VMEM((LEVELS, PAIRS, 2, LEAF, LEAF), BF),
            pltpu.VMEM((MERGED, PAIRS, 32, LEAF), BF),
            pltpu.VMEM((MERGED, PAIRS, 32, LEAF), BF),
            pltpu.VMEM((MERGED, PAIRS, LEAF, LEAF), BF),
            pltpu.VMEM((PAIRS, LEAF, 2 * LEAF), BF),
            pltpu.VMEM((2 * len(PLAN), GROUPS, CODE_ROWS, LEAF), jnp.int16),
            pltpu.VMEM((PARTNERS * GROUPS, CODE_ROWS, LEAF), jnp.int16),
            pltpu.VMEM((2 * len(PLAN), GROUPS, 8, LEAF), F32),
            pltpu.VMEM((PARTNERS * GROUPS, 8, LEAF), F32),
            pltpu.VMEM((CAP, 2 * RHS, LEAF), F32),
            pltpu.VMEM((BOXES + 2 * REACH, 2 * RHS, LEAF), F32),
            pltpu.VMEM((2, REACH, 2 * RHS, LEAF), F32),
            pltpu.SMEM((2, CAP), jnp.int32),
            pltpu.VMEM((SENT_ROWS, LEAF), BF),
            pltpu.SemaphoreType.DMA((7,)),
            pltpu.SemaphoreType.DMA,
            pltpu.SemaphoreType.DMA((COPIES,)),
        ],
        compiler_params=pltpu.CompilerParams(
            collective_id=0, has_side_effects=True, vmem_limit_bytes=56 * 1024 * 1024
        ),
        name="adjoint",
    )(near_list.T, signal, row_basis, transfer, column_basis, near_blocks)


def solution(mesh):
    return jax.shard_map(
        shards,
        mesh=mesh,
        in_specs=(
            P(None, ("leaf", "sub")),
            P(None, ("leaf", "sub")),
            P(("leaf", "sub"), None, None, None),
            P(None, ("leaf", "sub")),
            P(("leaf", "sub"), None, None),
            P(("leaf", "sub"), None),
        ),
        out_specs=P(None, ("leaf", "sub")),
        check_vma=False,
    )
```

```python
import functools

import jax
import jax.numpy as jnp
from jax import lax
from jax.experimental import pallas as pl
from jax.experimental.pallas import tpu as pltpu
from jax.sharding import PartitionSpec as P

LEAF = 128
BOXES = 16
PAIRS = 8
RHS = 16
CAP = 24
REACH = 4
LEVELS = 13
LOCAL = 4
GROUPS = 2
WIDTH = PAIRS // GROUPS
PHASES = (
    ((("sub", 0), ("sub", 1)), "receive"),
    ((("leaf", 0), ("leaf", 1)), "send"),
    ((("leaf", 2), ("leaf", 3)), "send"),
    ((("leaf", 4),), "one"),
    ((("leaf", 5), ("leaf", 6)), "send"),
)
FULL = 32767.0
SMALLEST = 1e-30
STEPS = 64.0

BF = jnp.bfloat16
F32 = jnp.float32
MESH = pl.DeviceIdType.MESH


def bit_of(index, bit):
    return (index // (1 << bit)) % 2


def flipped(index, bit):
    return index + (1 - 2 * bit_of(index, bit)) * (1 << bit)


def pieces(values):
    high = values.astype(BF)
    low = (values - high.astype(F32)).astype(BF)
    return jnp.concatenate([high, low], axis=0)


def folded(product):
    half = product.shape[0] // 2
    return product[:half] + product[half:]


def dot(left, right):
    return jnp.dot(left, right, preferred_element_type=F32)


def coded(coeffs):
    peak = jnp.abs(coeffs[0])
    for values in coeffs[1:]:
        peak = jnp.maximum(peak, jnp.abs(values))
    peak = jnp.maximum(jnp.maximum(peak[:8], peak[8:]), SMALLEST)
    power = jnp.ceil(jnp.log2(peak * (1.0 / FULL)) * STEPS + 0.125)
    inverse = jnp.exp2(power * (-1.0 / STEPS))
    inverse = jnp.concatenate([inverse, inverse], axis=0)
    codes = [jnp.round(values * inverse) for values in coeffs]
    codes.append(power)
    return [code.astype(jnp.int32).astype(jnp.int16) for code in codes]


def phase_plan():
    plan = []
    level = LOCAL
    slot = 0
    for bits, mode in PHASES:
        if mode == "one":
            plan.append((bits, level, mode, (bits,), None))
        else:
            low, high = bits
            plan.append((bits, level, mode, ((high,), (low, high), (low,)), slot))
            slot += 1
        level += len(bits)
    return tuple(plan), slot


PLAN, MERGED = phase_plan()
PARTNERS = sum(len(entry[3]) for entry in PLAN)
WEIGHTS = PARTNERS * GROUPS
HALO = WEIGHTS + MERGED
RIM = HALO + 2
COPIES = RIM + 2
CODE_ROWS = WIDTH * RHS + 8
SENT_ROWS = (
    PARTNERS * GROUPS * CODE_ROWS
    + MERGED * PAIRS * 32
    + 2 * 2 * REACH * 2 * RHS
    + 2 * REACH * 2 * RHS * 2
)


def kernel(
    list_hbm, sig_hbm, row_hbm, tr_hbm, col_hbm, near_hbm, out,
    sig, row, tr, col, near, window, mats, packed, far_tr, far_mats, basis, send_buf, recv_buf,
    products, field, rim, list_ref, tally, load_sem, push_sem, pull_sem,
):
    leaf = lax.axis_index("leaf")
    sub = lax.axis_index("sub")
    leaves = lax.axis_size("leaf")
    subs = lax.axis_size("sub")

    loads = [
        pltpu.make_async_copy(sig_hbm, sig, load_sem.at[0]),
        pltpu.make_async_copy(row_hbm, row, load_sem.at[1]),
        pltpu.make_async_copy(tr_hbm.at[:, : LOCAL + 1], tr.at[:, : LOCAL + 1], load_sem.at[2]),
        pltpu.make_async_copy(tr_hbm.at[:, LOCAL + 1 :], tr.at[:, LOCAL + 1 :], load_sem.at[3]),
        pltpu.make_async_copy(near_hbm, near, load_sem.at[4]),
        pltpu.make_async_copy(col_hbm, col, load_sem.at[5]),
        pltpu.make_async_copy(list_hbm, list_ref, load_sem.at[6]),
    ]
    for load in loads:
        load.start()

    def partner(bits):
        places = {"leaf": leaf, "sub": sub}
        for axis, bit in bits:
            places[axis] = flipped(places[axis], bit)
        return places["leaf"], places["sub"]

    def side(step, which):
        axis, bit = PLAN[step][0][which]
        return bit_of(leaf if axis == "leaf" else sub, bit)

    rank = leaf * subs + sub
    after = (rank + 1) % (leaves * subs)
    before = (rank + leaves * subs - 1) % (leaves * subs)
    after = (after // subs, after % subs)
    before = (before // subs, before % subs)

    peers = [partner(bits) for entry in PLAN for bits in entry[3]]
    peers += [after, before]
    barrier = pltpu.get_barrier_semaphore()
    for peer in peers:
        pl.semaphore_signal(barrier, inc=1, device_id=peer, device_id_type=MESH)

    lane = lax.broadcasted_iota(jnp.int32, (32, LEAF), 1)
    group = lane // 32
    odd = (group % 2).astype(F32)
    upper = (group // 2).astype(F32)
    odd_b = odd.astype(BF)
    even_b = (1.0 - odd).astype(BF)
    sign_b = (1.0 - 2.0 * odd).astype(BF)
    upper_b = upper.astype(BF)
    lower_b = (1.0 - upper).astype(BF)
    first_half = lax.broadcasted_iota(jnp.int32, (RHS, LEAF), 1) < 64

    def turned(weights):
        by32, by64, by96 = (pltpu.roll(weights, shift, 1) for shift in (32, 64, 96))
        return (
            weights * sign_b,
            by96 * even_b + by32 * odd_b,
            by64 * sign_b,
            by32 * even_b + by96 * odd_b,
        )

    def expand(source, target, pairs=(0, PAIRS)):
        def body(pair, carry):
            s0, c0, sr0, cr0 = turned(source(2 * pair))
            s1, c1, sr1, cr1 = turned(source(2 * pair + 1))
            target[pair, 0] = jnp.concatenate(
                [s0 * lower_b, c0 * lower_b, sr1 * upper_b, cr1 * upper_b], axis=0
            )
            target[pair, 1] = jnp.concatenate(
                [sr0 * lower_b, cr0 * lower_b, s1 * upper_b, c1 * upper_b], axis=0
            )
            return carry

        lax.fori_loop(*pairs, body, 0, unroll=8)

    def expand_first(source, target):
        def body(pair, carry):
            s0, c0, sr0, cr0 = turned(source(2 * pair))
            s1, c1, sr1, cr1 = turned(source(2 * pair + 1))
            target[pair, 0] = jnp.concatenate(
                [
                    s0 * lower_b + sr1 * upper_b,
                    c0 * lower_b + cr1 * upper_b,
                    sr0 * lower_b + s1 * upper_b,
                    cr0 * lower_b + c1 * upper_b,
                ],
                axis=0,
            )
            return carry

        lax.fori_loop(0, PAIRS, body, 0, unroll=8)

    def expand_level(level):
        expand(lambda box: tr[box, level], mats.at[level])

    for load in loads[:3]:
        load.wait()
    def remote(source, target, number, peer):
        return pltpu.make_async_remote_copy(
            src_ref=source, dst_ref=target, send_sem=push_sem,
            recv_sem=pull_sem.at[number], device_id=peer, device_id_type=MESH,
        )

    weight_copies = {}
    for step, (_, _, mode, sets, slot) in enumerate(PLAN):
        if slot is not None:
            weight_copies[slot] = remote(
                packed.at[slot], far_tr.at[slot], WEIGHTS + slot,
                partner(sets[0] if mode == "receive" else sets[2]),
            )

    def pack(step):
        _, level, _, _, slot = PLAN[step]
        upper_child = (1 - side(step, 0)).astype(F32)
        straight = ((1.0 - upper) * (1.0 - upper_child)).astype(BF)
        straight_next = (upper * upper_child).astype(BF)
        turned_round = ((1.0 - upper) * upper_child).astype(BF)
        turned_next = (upper * (1.0 - upper_child)).astype(BF)
        for pair in range(PAIRS):
            one, two = tr[2 * pair, level], tr[2 * pair + 1, level]
            packed[slot, pair] = (
                one * straight
                + pltpu.roll(one, 64, 1) * turned_round
                + two * straight_next
                + pltpu.roll(two, 64, 1) * turned_next
            )

    pack(0)
    coeffs = []
    for pair in range(PAIRS):
        left, right = [], []
        for box in (2 * pair, 2 * pair + 1):
            points = slice(box * LEAF, (box + 1) * LEAF)
            samples = sig[:, points]
            window[2 * REACH + box] = samples
            left.append(jnp.concatenate([samples[:RHS], samples[RHS:]], axis=1))
            real, imag = row[:32, points], row[32:, points]
            right.append(
                jnp.concatenate(
                    [jnp.concatenate([real, imag], axis=1), jnp.concatenate([-imag, real], axis=1)],
                    axis=0,
                )
            )
        product = lax.dot_general(
            jnp.concatenate(left, axis=0), jnp.concatenate(right, axis=0),
            (((1,), (1,)), ((), ())), preferred_element_type=F32,
        )
        coeffs.append(jnp.where(first_half, product[:RHS], product[RHS:]))

    expand_first(lambda box: tr[box, 0], mats.at[0])
    for level in range(1, LOCAL + 1):
        expand_level(level)

    pl.semaphore_wait(barrier, len(peers))
    weight_copies[0].start()

    coeffs = [folded(dot(pieces(coeffs[pair]), mats[0, pair, 0])) for pair in range(PAIRS)]
    for level in range(1, LOCAL):
        span = 1 << (level - 1)
        split = [pieces(values) for values in coeffs]
        following = []
        for pair in range(PAIRS):
            low = pair & ~span
            joined = jnp.concatenate([split[low], split[low | span]], axis=1)
            weights = mats[level, pair].reshape(2 * LEAF, LEAF)
            following.append(folded(dot(joined, weights)))
        coeffs = following

    edge = 2 * REACH
    halo = (
        remote(window.at[BOXES : BOXES + edge], window.at[:edge], HALO, after),
        remote(window.at[edge : 2 * edge], window.at[edge + BOXES :], HALO + 1, before),
    )

    def send_halo():
        for copy in halo:
            copy.start()

    def near_field():
        for copy in halo:
            copy.wait_recv()
        loads[4].wait()
        loads[6].wait()

        def multiply(slot, carry):
            picked = window[jnp.maximum(list_ref[0, slot], 0)]
            product = dot(picked, near[slot])
            real = product[:RHS, :LEAF] + product[RHS:, LEAF:]
            imag = product[RHS:, :LEAF] - product[:RHS, LEAF:]
            products[slot] = jnp.concatenate([real, imag], axis=0)
            return carry

        lax.fori_loop(0, CAP, multiply, 0, unroll=8)

        def gather(box, carry):
            total = jnp.zeros((2 * RHS, LEAF), F32)
            for slot in range(CAP):
                here = jnp.where(list_ref[1, slot] == box, 1.0, 0.0).astype(F32)
                total += products[slot] * here
            field[box] = total
            return carry

        lax.fori_loop(0, BOXES + 2 * REACH, gather, 0)

    rims = (
        remote(field.at[:REACH], rim.at[0], RIM, before),
        remote(field.at[BOXES + REACH :], rim.at[1], RIM + 1, after),
    )

    def send_rims():
        for copy in rims:
            copy.start()

    def expand_basis():
        loads[5].wait()
        for box in range(BOXES):
            points = slice(box * LEAF, (box + 1) * LEAF)
            real, imag = col[:32, points], col[32:, points]
            basis[box // 2, 64 * (box % 2) : 64 * (box % 2) + 64] = jnp.concatenate(
                [jnp.concatenate([real, imag], axis=1), jnp.concatenate([-imag, real], axis=1)],
                axis=0,
            )

    def finish_near():
        for copy in rims:
            copy.wait_recv()
        for place in range(REACH):
            field[REACH + place] += rim[1, place]
            field[BOXES + place] += rim[0, place]

    def finish(pair, values):
        zero = jnp.zeros_like(values)
        left = jnp.concatenate(
            [pieces(jnp.where(first_half, values, zero)), pieces(jnp.where(first_half, zero, values))],
            axis=0,
        )
        product = dot(left, basis[pair])
        for half in range(2):
            far_box = folded(product[2 * RHS * half : 2 * RHS * (half + 1)])
            box = 2 * pair + half
            points = slice(box * LEAF, (box + 1) * LEAF)
            near_box = field[REACH + box]
            out[:RHS, points] = far_box[:, :LEAF] + near_box[:RHS]
            out[RHS:, points] = far_box[:, LEAF:] + near_box[RHS:]

    def expand_far(slot):
        weight_copies[slot].wait_recv()
        for pair in range(PAIRS):
            weights = far_tr[slot, pair]
            signed = weights * sign_b
            crossed = pltpu.roll(weights, 96, 1) * even_b + pltpu.roll(weights, 32, 1) * odd_b
            far_mats[slot, pair] = jnp.concatenate(
                [signed * lower_b, crossed * lower_b, signed * upper_b, crossed * upper_b], axis=0
            )

    def fill(step):
        if step == 0:
            loads[3].wait()
            for later in range(1, len(PLAN)):
                if PLAN[later][4] is not None:
                    pack(later)
                    weight_copies[PLAN[later][4]].start()
            for level in range(LOCAL + 1, LEVELS):
                expand_level(level)
            expand_basis()
            expand_far(1)
            expand_far(0)
        elif step == 1:
            send_halo()
            expand_far(2)
        elif step == 2:
            expand_far(3)
            near_field()
            send_rims()

    first_number = []
    total = 0
    for entry in PLAN:
        first_number.append(total)
        total += len(entry[3])

    def number_of(step, group, order):
        return GROUPS * (first_number[step] + order) + group

    def message(step, group, which, order):
        number = number_of(step, group, order)
        return remote(
            send_buf.at[2 * step + which, group], recv_buf.at[number], number,
            partner(PLAN[step][3][order]),
        )

    def push(step, group, which, values, orders):
        *codes, power = coded(values)
        for index, code in enumerate(codes):
            send_buf[2 * step + which, group, RHS * index : RHS * (index + 1)] = code
        send_buf[2 * step + which, group, WIDTH * RHS :] = power
        for order in orders:
            message(step, group, which, order).start()

    def arrived(step, group, order):
        number = number_of(step, group, order)
        message(step, group, 0, order).wait_recv()
        tiles = [
            recv_buf[number, RHS * index : RHS * (index + 1)].astype(F32)
            for index in range(WIDTH)
        ]
        scale = jnp.exp2(recv_buf[number, WIDTH * RHS :].astype(F32) * (1.0 / STEPS))
        scale = jnp.concatenate([scale, scale], axis=0)
        return [tile * scale for tile in tiles]

    def times(values, weights):
        return [folded(dot(pieces(values[index]), weights(index))) for index in range(WIDTH)]

    def sums(left, right):
        return [one + two for one, two in zip(left, right)]

    def matrices(level, group, child):
        return lambda index: mats[level, WIDTH * group + index, child]

    def send(step, group, values):
        _, level, mode, _, slot = PLAN[step]
        mine = matrices(level, group, side(step, 0))
        if mode == "one":
            push(step, group, 0, values, (0,))
            return lambda: times(values, mine)
        if mode == "receive":
            push(step, group, 0, values, (1, 2))
            own = times(values, mine)
            push(step, group, 1, own, (0,))
            return lambda: own
        both = [
            folded(
                dot(
                    pieces(values[index]),
                    jnp.concatenate(
                        [mine(index), far_mats[slot, WIDTH * group + index]], axis=1
                    ),
                )
            )
            for index in range(WIDTH)
        ]
        own = [value[:, :LEAF] for value in both]
        push(step, group, 1, own, (0,))
        push(step, group, 0, [value[:, LEAF:] for value in both], (1, 2))
        return lambda: own

    coeffs = [coeffs[WIDTH * group : WIDTH * (group + 1)] for group in range(GROUPS)]
    partial = [send(0, group, coeffs[group])() for group in range(GROUPS)]
    for step, (bits, level, mode, sets, slot) in enumerate(PLAN):
        fill(step)
        for group in range(GROUPS):
            other = matrices(level, group, 1 - side(step, 0))
            if mode == "one":
                values = sums(partial[group], times(arrived(step, group, 0), other))
            else:
                values = arrived(step, group, 2)
                if mode == "receive":
                    values = times(values, other)
                values = sums(partial[group], values)
                mine_next = side(step, 1)
                first = matrices(level + 1, group, mine_next)
                second = matrices(level + 1, group, 1 - mine_next)
                if group == 0:
                    ahead = times(values, first)
                far = arrived(step, group, 1)
                if mode == "receive":
                    far = times(far, lambda index: far_mats[slot, WIDTH * group + index])
                far = sums(far, arrived(step, group, 0))
                if group == 0:
                    values = sums(ahead, times(far, second))
                else:
                    values = [
                        folded(
                            dot(
                                jnp.concatenate([pieces(values[index]), pieces(far[index])], axis=1),
                                jnp.concatenate([first(index), second(index)], axis=0),
                            )
                        )
                        for index in range(WIDTH)
                    ]
            coeffs[group] = values
            if step + 1 < len(PLAN):
                partial[group] = send(step + 1, group, values)()
            else:
                if group == 0:
                    finish_near()
                for index in range(WIDTH):
                    finish(WIDTH * group + index, values[index])

    pltpu.make_async_copy(tally, tally, push_sem).wait()


def shards(signal, row_basis, transfer, column_basis, near_blocks, near_list):
    anywhere = pl.BlockSpec(memory_space=pltpu.HBM)
    return pl.pallas_call(
        kernel,
        out_shape=pltpu.VMEM((2 * RHS, BOXES * LEAF), F32),
        in_specs=[anywhere] * 6,
        out_specs=pl.BlockSpec(memory_space=pltpu.VMEM),
        scratch_shapes=[
            pltpu.VMEM((2 * RHS, BOXES * LEAF), BF),
            pltpu.VMEM((64, BOXES * LEAF), BF),
            pltpu.VMEM((BOXES, LEVELS, 32, LEAF), BF),
            pltpu.VMEM((64, BOXES * LEAF), BF),
            pltpu.VMEM((CAP, LEAF, 2 * LEAF), BF),
            pltpu.VMEM((BOXES + 4 * REACH, 2 * RHS, LEAF), BF),
            pltpu.VMEM((LEVELS, PAIRS, 2, LEAF, LEAF), BF),
            pltpu.VMEM((MERGED, PAIRS, 32, LEAF), BF),
            pltpu.VMEM((MERGED, PAIRS, 32, LEAF), BF),
            pltpu.VMEM((MERGED, PAIRS, LEAF, LEAF), BF),
            pltpu.VMEM((PAIRS, LEAF, 2 * LEAF), BF),
            pltpu.VMEM((2 * len(PLAN), GROUPS, CODE_ROWS, LEAF), jnp.int16),
            pltpu.VMEM((PARTNERS * GROUPS, CODE_ROWS, LEAF), jnp.int16),
            pltpu.VMEM((CAP, 2 * RHS, LEAF), F32),
            pltpu.VMEM((BOXES + 2 * REACH, 2 * RHS, LEAF), F32),
            pltpu.VMEM((2, REACH, 2 * RHS, LEAF), F32),
            pltpu.SMEM((2, CAP), jnp.int32),
            pltpu.VMEM((SENT_ROWS, LEAF), BF),
            pltpu.SemaphoreType.DMA((7,)),
            pltpu.SemaphoreType.DMA,
            pltpu.SemaphoreType.DMA((COPIES,)),
        ],
        compiler_params=pltpu.CompilerParams(
            collective_id=0, has_side_effects=True, vmem_limit_bytes=56 * 1024 * 1024
        ),
        name="adjoint",
    )(near_list.T, signal, row_basis, transfer, column_basis, near_blocks)


def solution(mesh):
    return jax.shard_map(
        shards,
        mesh=mesh,
        in_specs=(
            P(None, ("leaf", "sub")),
            P(None, ("leaf", "sub")),
            P(("leaf", "sub"), None, None, None),
            P(None, ("leaf", "sub")),
            P(("leaf", "sub"), None, None),
            P(("leaf", "sub"), None),
        ),
        out_specs=P(None, ("leaf", "sub")),
        check_vma=False,
    )
```

```python
import functools

import jax
import jax.numpy as jnp
from jax import lax
from jax.experimental import pallas as pl
from jax.experimental.pallas import tpu as pltpu
from jax.sharding import PartitionSpec as P

LEAF = 128
BOXES = 16
PAIRS = 8
RHS = 16
CAP = 24
REACH = 4
LEVELS = 13
LOCAL = 4
GROUPS = 2
WIDTH = PAIRS // GROUPS
PHASES = (
    ((("sub", 0), ("sub", 1)), "receive"),
    ((("leaf", 0), ("leaf", 1)), "send"),
    ((("leaf", 2), ("leaf", 3)), "send"),
    ((("leaf", 4),), "one"),
    ((("leaf", 5), ("leaf", 6)), "send"),
)
FULL = 32767.0
SMALLEST = 1e-30
STEPS = 64.0

BF = jnp.bfloat16
F32 = jnp.float32
MESH = pl.DeviceIdType.MESH


def bit_of(index, bit):
    return (index // (1 << bit)) % 2


def flipped(index, bit):
    return index + (1 - 2 * bit_of(index, bit)) * (1 << bit)


def pieces(values):
    high = values.astype(BF)
    low = (values - high.astype(F32)).astype(BF)
    return jnp.concatenate([high, low], axis=0)


def folded(product):
    half = product.shape[0] // 2
    return product[:half] + product[half:]


def dot(left, right):
    return jnp.dot(left, right, preferred_element_type=F32)


def coded(coeffs):
    peak = jnp.abs(coeffs[0])
    for values in coeffs[1:]:
        peak = jnp.maximum(peak, jnp.abs(values))
    peak = jnp.maximum(jnp.maximum(peak[:8], peak[8:]), SMALLEST)
    power = jnp.ceil(jnp.log2(peak * (1.0 / FULL)) * STEPS + 0.125)
    inverse = jnp.exp2(power * (-1.0 / STEPS))
    inverse = jnp.concatenate([inverse, inverse], axis=0)
    codes = [jnp.round(values * inverse) for values in coeffs]
    codes.append(power)
    return [code.astype(jnp.int32).astype(jnp.int16) for code in codes]


def phase_plan():
    plan = []
    level = LOCAL
    slot = 0
    for bits, mode in PHASES:
        if mode == "one":
            plan.append((bits, level, mode, (bits,), None))
        else:
            low, high = bits
            plan.append((bits, level, mode, ((high,), (low, high), (low,)), slot))
            slot += 1
        level += len(bits)
    return tuple(plan), slot


PLAN, MERGED = phase_plan()
PARTNERS = sum(len(entry[3]) for entry in PLAN)
WEIGHTS = PARTNERS * GROUPS
HALO = WEIGHTS + MERGED * GROUPS
RIM = HALO + 2
COPIES = RIM + 2
CODE_ROWS = WIDTH * RHS + 8
SENT_ROWS = (
    PARTNERS * GROUPS * CODE_ROWS
    + MERGED * PAIRS * 32
    + 2 * 2 * REACH * 2 * RHS
    + 2 * REACH * 2 * RHS * 2
)


def kernel(
    list_hbm, sig_hbm, row_hbm, tr_hbm, col_hbm, near_hbm, out,
    sig, row, tr, col, near, window, mats, packed, far_tr, far_mats, basis, send_buf, recv_buf,
    products, field, rim, list_ref, tally, load_sem, push_sem, pull_sem,
):
    leaf = lax.axis_index("leaf")
    sub = lax.axis_index("sub")
    leaves = lax.axis_size("leaf")
    subs = lax.axis_size("sub")

    loads = [
        pltpu.make_async_copy(sig_hbm, sig, load_sem.at[0]),
        pltpu.make_async_copy(row_hbm, row, load_sem.at[1]),
        pltpu.make_async_copy(tr_hbm.at[:, : LOCAL + 1], tr.at[:, : LOCAL + 1], load_sem.at[2]),
        pltpu.make_async_copy(tr_hbm.at[:, LOCAL + 1 :], tr.at[:, LOCAL + 1 :], load_sem.at[3]),
        pltpu.make_async_copy(near_hbm, near, load_sem.at[4]),
        pltpu.make_async_copy(col_hbm, col, load_sem.at[5]),
        pltpu.make_async_copy(list_hbm, list_ref, load_sem.at[6]),
    ]
    for load in loads:
        load.start()

    def partner(bits):
        places = {"leaf": leaf, "sub": sub}
        for axis, bit in bits:
            places[axis] = flipped(places[axis], bit)
        return places["leaf"], places["sub"]

    def side(step, which):
        axis, bit = PLAN[step][0][which]
        return bit_of(leaf if axis == "leaf" else sub, bit)

    rank = leaf * subs + sub
    after = (rank + 1) % (leaves * subs)
    before = (rank + leaves * subs - 1) % (leaves * subs)
    after = (after // subs, after % subs)
    before = (before // subs, before % subs)

    peers = [partner(bits) for entry in PLAN for bits in entry[3]]
    peers += [after, before]
    barrier = pltpu.get_barrier_semaphore()
    for peer in peers:
        pl.semaphore_signal(barrier, inc=1, device_id=peer, device_id_type=MESH)

    lane = lax.broadcasted_iota(jnp.int32, (32, LEAF), 1)
    group = lane // 32
    odd = (group % 2).astype(F32)
    upper = (group // 2).astype(F32)
    odd_b = odd.astype(BF)
    even_b = (1.0 - odd).astype(BF)
    sign_b = (1.0 - 2.0 * odd).astype(BF)
    upper_b = upper.astype(BF)
    lower_b = (1.0 - upper).astype(BF)
    first_half = lax.broadcasted_iota(jnp.int32, (RHS, LEAF), 1) < 64

    def turned(weights):
        by32, by64, by96 = (pltpu.roll(weights, shift, 1) for shift in (32, 64, 96))
        return (
            weights * sign_b,
            by96 * even_b + by32 * odd_b,
            by64 * sign_b,
            by32 * even_b + by96 * odd_b,
        )

    def expand(source, target, pairs=(0, PAIRS)):
        def body(pair, carry):
            s0, c0, sr0, cr0 = turned(source(2 * pair))
            s1, c1, sr1, cr1 = turned(source(2 * pair + 1))
            target[pair, 0] = jnp.concatenate(
                [s0 * lower_b, c0 * lower_b, sr1 * upper_b, cr1 * upper_b], axis=0
            )
            target[pair, 1] = jnp.concatenate(
                [sr0 * lower_b, cr0 * lower_b, s1 * upper_b, c1 * upper_b], axis=0
            )
            return carry

        lax.fori_loop(*pairs, body, 0, unroll=8)

    def expand_first(source, target):
        def body(pair, carry):
            s0, c0, sr0, cr0 = turned(source(2 * pair))
            s1, c1, sr1, cr1 = turned(source(2 * pair + 1))
            target[pair, 0] = jnp.concatenate(
                [
                    s0 * lower_b + sr1 * upper_b,
                    c0 * lower_b + cr1 * upper_b,
                    sr0 * lower_b + s1 * upper_b,
                    cr0 * lower_b + c1 * upper_b,
                ],
                axis=0,
            )
            return carry

        lax.fori_loop(0, PAIRS, body, 0, unroll=8)

    def expand_level(level):
        expand(lambda box: tr[box, level], mats.at[level])

    for load in loads[:3]:
        load.wait()
    def remote(source, target, number, peer):
        return pltpu.make_async_remote_copy(
            src_ref=source, dst_ref=target, send_sem=push_sem,
            recv_sem=pull_sem.at[number], device_id=peer, device_id_type=MESH,
        )

    weight_copies = {}
    for step, (_, _, mode, sets, slot) in enumerate(PLAN):
        if slot is not None:
            for group in range(GROUPS):
                pairs = pl.ds(WIDTH * group, WIDTH)
                weight_copies[slot, group] = remote(
                    packed.at[slot, pairs], far_tr.at[slot, pairs],
                    WEIGHTS + GROUPS * slot + group,
                    partner(sets[0] if mode == "receive" else sets[2]),
                )

    def pack(step):
        _, level, _, _, slot = PLAN[step]
        upper_child = (1 - side(step, 0)).astype(F32)
        straight = ((1.0 - upper) * (1.0 - upper_child)).astype(BF)
        straight_next = (upper * upper_child).astype(BF)
        turned_round = ((1.0 - upper) * upper_child).astype(BF)
        turned_next = (upper * (1.0 - upper_child)).astype(BF)
        for pair in range(PAIRS):
            one, two = tr[2 * pair, level], tr[2 * pair + 1, level]
            packed[slot, pair] = (
                one * straight
                + pltpu.roll(one, 64, 1) * turned_round
                + two * straight_next
                + pltpu.roll(two, 64, 1) * turned_next
            )

    pack(0)
    coeffs = []
    for pair in range(PAIRS):
        left, right = [], []
        for box in (2 * pair, 2 * pair + 1):
            points = slice(box * LEAF, (box + 1) * LEAF)
            samples = sig[:, points]
            window[2 * REACH + box] = samples
            left.append(jnp.concatenate([samples[:RHS], samples[RHS:]], axis=1))
            real, imag = row[:32, points], row[32:, points]
            right.append(
                jnp.concatenate(
                    [jnp.concatenate([real, imag], axis=1), jnp.concatenate([-imag, real], axis=1)],
                    axis=0,
                )
            )
        product = lax.dot_general(
            jnp.concatenate(left, axis=0), jnp.concatenate(right, axis=0),
            (((1,), (1,)), ((), ())), preferred_element_type=F32,
        )
        coeffs.append(jnp.where(first_half, product[:RHS], product[RHS:]))

    expand_first(lambda box: tr[box, 0], mats.at[0])
    for level in range(1, LOCAL + 1):
        expand_level(level)

    pl.semaphore_wait(barrier, len(peers))
    for group in range(GROUPS):
        weight_copies[0, group].start()

    coeffs = [folded(dot(pieces(coeffs[pair]), mats[0, pair, 0])) for pair in range(PAIRS)]
    for level in range(1, LOCAL):
        span = 1 << (level - 1)
        split = [pieces(values) for values in coeffs]
        following = []
        for pair in range(PAIRS):
            low = pair & ~span
            joined = jnp.concatenate([split[low], split[low | span]], axis=1)
            weights = mats[level, pair].reshape(2 * LEAF, LEAF)
            following.append(folded(dot(joined, weights)))
        coeffs = following

    edge = 2 * REACH
    halo = (
        remote(window.at[BOXES : BOXES + edge], window.at[:edge], HALO, after),
        remote(window.at[edge : 2 * edge], window.at[edge + BOXES :], HALO + 1, before),
    )

    def send_halo():
        for copy in halo:
            copy.start()

    def near_field():
        for copy in halo:
            copy.wait_recv()
        loads[4].wait()
        loads[6].wait()

        def multiply(slot, carry):
            picked = window[jnp.maximum(list_ref[0, slot], 0)]
            product = dot(picked, near[slot])
            real = product[:RHS, :LEAF] + product[RHS:, LEAF:]
            imag = product[RHS:, :LEAF] - product[:RHS, LEAF:]
            products[slot] = jnp.concatenate([real, imag], axis=0)
            return carry

        lax.fori_loop(0, CAP, multiply, 0, unroll=8)

        def gather(box, carry):
            total = jnp.zeros((2 * RHS, LEAF), F32)
            for slot in range(CAP):
                here = jnp.where(list_ref[1, slot] == box, 1.0, 0.0).astype(F32)
                total += products[slot] * here
            field[box] = total
            return carry

        lax.fori_loop(0, BOXES + 2 * REACH, gather, 0)

    rims = (
        remote(field.at[:REACH], rim.at[0], RIM, before),
        remote(field.at[BOXES + REACH :], rim.at[1], RIM + 1, after),
    )

    def send_rims():
        for copy in rims:
            copy.start()

    def expand_basis():
        loads[5].wait()
        for box in range(BOXES):
            points = slice(box * LEAF, (box + 1) * LEAF)
            real, imag = col[:32, points], col[32:, points]
            basis[box // 2, 64 * (box % 2) : 64 * (box % 2) + 64] = jnp.concatenate(
                [jnp.concatenate([real, imag], axis=1), jnp.concatenate([-imag, real], axis=1)],
                axis=0,
            )

    def finish_near():
        for copy in rims:
            copy.wait_recv()
        for place in range(REACH):
            field[REACH + place] += rim[1, place]
            field[BOXES + place] += rim[0, place]

    def finish(pair, values):
        zero = jnp.zeros_like(values)
        left = jnp.concatenate(
            [pieces(jnp.where(first_half, values, zero)), pieces(jnp.where(first_half, zero, values))],
            axis=0,
        )
        product = dot(left, basis[pair])
        for half in range(2):
            far_box = folded(product[2 * RHS * half : 2 * RHS * (half + 1)])
            box = 2 * pair + half
            points = slice(box * LEAF, (box + 1) * LEAF)
            near_box = field[REACH + box]
            out[:RHS, points] = far_box[:, :LEAF] + near_box[:RHS]
            out[RHS:, points] = far_box[:, LEAF:] + near_box[RHS:]

    def expand_far(slot, groups=range(GROUPS)):
        for group in groups:
            weight_copies[slot, group].wait_recv()
        for pair in range(WIDTH * groups[0], WIDTH * (groups[-1] + 1)):
            weights = far_tr[slot, pair]
            signed = weights * sign_b
            crossed = pltpu.roll(weights, 96, 1) * even_b + pltpu.roll(weights, 32, 1) * odd_b
            far_mats[slot, pair] = jnp.concatenate(
                [signed * lower_b, crossed * lower_b, signed * upper_b, crossed * upper_b], axis=0
            )

    def fill(step):
        if step == 0:
            loads[3].wait()
            for later in range(1, len(PLAN)):
                if PLAN[later][4] is not None:
                    pack(later)
                    for group in range(GROUPS):
                        weight_copies[PLAN[later][4], group].start()
            for level in range(LOCAL + 1, LEVELS):
                expand_level(level)
            expand_basis()
            expand_far(1)
        elif step == 1:
            send_halo()
            expand_far(2)
        elif step == 2:
            expand_far(3)
            near_field()
            send_rims()

    first_number = []
    total = 0
    for entry in PLAN:
        first_number.append(total)
        total += len(entry[3])

    def number_of(step, group, order):
        return GROUPS * (first_number[step] + order) + group

    def message(step, group, which, order):
        number = number_of(step, group, order)
        return remote(
            send_buf.at[2 * step + which, group], recv_buf.at[number], number,
            partner(PLAN[step][3][order]),
        )

    def push(step, group, which, values, orders):
        *codes, power = coded(values)
        for index, code in enumerate(codes):
            send_buf[2 * step + which, group, RHS * index : RHS * (index + 1)] = code
        send_buf[2 * step + which, group, WIDTH * RHS :] = power
        for order in orders:
            message(step, group, which, order).start()

    def arrived(step, group, order):
        number = number_of(step, group, order)
        message(step, group, 0, order).wait_recv()
        tiles = [
            recv_buf[number, RHS * index : RHS * (index + 1)].astype(F32)
            for index in range(WIDTH)
        ]
        scale = jnp.exp2(recv_buf[number, WIDTH * RHS :].astype(F32) * (1.0 / STEPS))
        scale = jnp.concatenate([scale, scale], axis=0)
        return [tile * scale for tile in tiles]

    def times(values, weights):
        return [folded(dot(pieces(values[index]), weights(index))) for index in range(WIDTH)]

    def sums(left, right):
        return [one + two for one, two in zip(left, right)]

    def matrices(level, group, child):
        return lambda index: mats[level, WIDTH * group + index, child]

    def send(step, group, values):
        _, level, mode, _, slot = PLAN[step]
        mine = matrices(level, group, side(step, 0))
        if mode == "one":
            push(step, group, 0, values, (0,))
            return lambda: times(values, mine)
        if mode == "receive":
            push(step, group, 0, values, (1, 2))
            own = times(values, mine)
            push(step, group, 1, own, (0,))
            return lambda: own
        both = [
            folded(
                dot(
                    pieces(values[index]),
                    jnp.concatenate(
                        [mine(index), far_mats[slot, WIDTH * group + index]], axis=1
                    ),
                )
            )
            for index in range(WIDTH)
        ]
        own = [value[:, :LEAF] for value in both]
        push(step, group, 1, own, (0,))
        push(step, group, 0, [value[:, LEAF:] for value in both], (1, 2))
        return lambda: own

    coeffs = [coeffs[WIDTH * group : WIDTH * (group + 1)] for group in range(GROUPS)]
    partial = [send(0, group, coeffs[group])() for group in range(GROUPS)]
    for step, (bits, level, mode, sets, slot) in enumerate(PLAN):
        fill(step)
        for group in range(GROUPS):
            other = matrices(level, group, 1 - side(step, 0))
            if step == 0:
                expand_far(0, (group,))
            if mode == "one":
                values = sums(partial[group], times(arrived(step, group, 0), other))
            else:
                values = arrived(step, group, 2)
                if mode == "receive":
                    values = times(values, other)
                values = sums(partial[group], values)
                mine_next = side(step, 1)
                first = matrices(level + 1, group, mine_next)
                second = matrices(level + 1, group, 1 - mine_next)
                if group == 0:
                    ahead = times(values, first)
                far = arrived(step, group, 1)
                if mode == "receive":
                    far = times(far, lambda index: far_mats[slot, WIDTH * group + index])
                far = sums(far, arrived(step, group, 0))
                if group == 0:
                    values = sums(ahead, times(far, second))
                else:
                    values = [
                        folded(
                            dot(
                                jnp.concatenate([pieces(values[index]), pieces(far[index])], axis=1),
                                jnp.concatenate([first(index), second(index)], axis=0),
                            )
                        )
                        for index in range(WIDTH)
                    ]
            coeffs[group] = values
            if step + 1 < len(PLAN):
                partial[group] = send(step + 1, group, values)()
            else:
                if group == 0:
                    finish_near()
                for index in range(WIDTH):
                    finish(WIDTH * group + index, values[index])

    pltpu.make_async_copy(tally, tally, push_sem).wait()


def shards(signal, row_basis, transfer, column_basis, near_blocks, near_list):
    anywhere = pl.BlockSpec(memory_space=pltpu.HBM)
    return pl.pallas_call(
        kernel,
        out_shape=pltpu.VMEM((2 * RHS, BOXES * LEAF), F32),
        in_specs=[anywhere] * 6,
        out_specs=pl.BlockSpec(memory_space=pltpu.VMEM),
        scratch_shapes=[
            pltpu.VMEM((2 * RHS, BOXES * LEAF), BF),
            pltpu.VMEM((64, BOXES * LEAF), BF),
            pltpu.VMEM((BOXES, LEVELS, 32, LEAF), BF),
            pltpu.VMEM((64, BOXES * LEAF), BF),
            pltpu.VMEM((CAP, LEAF, 2 * LEAF), BF),
            pltpu.VMEM((BOXES + 4 * REACH, 2 * RHS, LEAF), BF),
            pltpu.VMEM((LEVELS, PAIRS, 2, LEAF, LEAF), BF),
            pltpu.VMEM((MERGED, PAIRS, 32, LEAF), BF),
            pltpu.VMEM((MERGED, PAIRS, 32, LEAF), BF),
            pltpu.VMEM((MERGED, PAIRS, LEAF, LEAF), BF),
            pltpu.VMEM((PAIRS, LEAF, 2 * LEAF), BF),
            pltpu.VMEM((2 * len(PLAN), GROUPS, CODE_ROWS, LEAF), jnp.int16),
            pltpu.VMEM((PARTNERS * GROUPS, CODE_ROWS, LEAF), jnp.int16),
            pltpu.VMEM((CAP, 2 * RHS, LEAF), F32),
            pltpu.VMEM((BOXES + 2 * REACH, 2 * RHS, LEAF), F32),
            pltpu.VMEM((2, REACH, 2 * RHS, LEAF), F32),
            pltpu.SMEM((2, CAP), jnp.int32),
            pltpu.VMEM((SENT_ROWS, LEAF), BF),
            pltpu.SemaphoreType.DMA((7,)),
            pltpu.SemaphoreType.DMA,
            pltpu.SemaphoreType.DMA((COPIES,)),
        ],
        compiler_params=pltpu.CompilerParams(
            collective_id=0, has_side_effects=True, vmem_limit_bytes=56 * 1024 * 1024
        ),
        name="adjoint",
    )(near_list.T, signal, row_basis, transfer, column_basis, near_blocks)


def solution(mesh):
    return jax.shard_map(
        shards,
        mesh=mesh,
        in_specs=(
            P(None, ("leaf", "sub")),
            P(None, ("leaf", "sub")),
            P(("leaf", "sub"), None, None, None),
            P(None, ("leaf", "sub")),
            P(("leaf", "sub"), None, None),
            P(("leaf", "sub"), None),
        ),
        out_specs=P(None, ("leaf", "sub")),
        check_vma=False,
    )
```
